8 devices in a mesh: dp: 2 (over y, z), tp: 4 (over x, core).
Axes of the slice: x: 2, y: 2, z: 1, core: 2. Of those that a mesh axis runs over, the one named last changes fastest.
Arguments:
- x: bfloat16 [4096, 2304], P(('dp', 'tp')), parts along dimension 0
- dy: bfloat16 [4096, 2304], P(('dp', 'tp')), parts along dimension 0
- gain: bfloat16 [2304], replicated
- wq: bfloat16 [2304, 2048], P(None, 'tp')
- wk: bfloat16 [2304, 1024], P(None, 'tp')
- wv: bfloat16 [2304, 1024], P(None, 'tp')
- wo: bfloat16 [2048, 2304], P('tp')
Outputs:
- output 1: bfloat16 [4096, 2304], P(('dp', 'tp')), parts along dimension 0
- output 2: float32 [2, 2304], P('dp'), parts along dimension 0
- output 3: bfloat16 [4608, 2048], P('dp', 'tp'), parts along dimension 0
- output 4: bfloat16 [4608, 1024], P('dp', 'tp'), parts along dimension 0
- output 5: bfloat16 [4608, 1024], P('dp', 'tp'), parts along dimension 0
- output 6: bfloat16 [4096, 2304], P(('dp', 'tp')), parts along dimension 0
There are 2 independent parts. The reference program is written for one: setup_inputs(seed, part) draws one part's arguments, and reference() takes and returns one part's arrays. A program takes and returns all parts, laid end to end along the dimension named above; an argument that names none is the same for every part.
All inputs are finite; a program needn't handle non-finite values.
Results may differ from the reference program's by a relative error of at most 0.018.
Values are sent between devices in bfloat16 or wider.
A program may use at most 2 GiB of HBM per device.

```python
import jax
import jax.numpy as jnp
from jax import lax

ROWS = 2048
D = 2304
HEADS = 8
KV_HEADS = 4
HEAD = 256
THETA = 10000


def setup_inputs(seed: int = 0, part: int = 0) -> dict:
    kx, ky, kn, kq, kk, kv, ko = jax.random.split(jax.random.key(seed), 7)

    def weights(key, rows, columns):
        return jax.random.normal(key, (rows, columns), jnp.float32) * rows**-0.5

    drawn = {
        "x": jax.random.normal(jax.random.fold_in(kx, part), (ROWS, D), jnp.float32),
        "dy": jax.random.normal(jax.random.fold_in(ky, part), (ROWS, D), jnp.float32) * ROWS**-0.5,
        "gain": 1 + 0.1 * jax.random.normal(kn, (D,), jnp.float32),
        "wq": 2 * weights(kq, D, HEADS * HEAD),
        "wk": 2 * weights(kk, D, KV_HEADS * HEAD),
        "wv": 4 * weights(kv, D, KV_HEADS * HEAD),
        "wo": weights(ko, HEADS * HEAD, D),
    }
    return {k: v.astype(jnp.bfloat16) for k, v in drawn.items()}


def normed(x, gain):
    wide = x.astype(jnp.float32)
    scale = lax.rsqrt(jnp.mean(wide * wide, -1, keepdims=True) + 1e-6)
    return (wide * scale * gain.astype(jnp.float32)).astype(jnp.bfloat16)


def turned(t, place, theta):
    half = t.shape[-1] // 2
    angle = place.astype(jnp.float32)[:, None] * theta ** (-jnp.arange(half, dtype=jnp.float32) / half)
    cos, sin = jnp.cos(angle)[:, None], jnp.sin(angle)[:, None]
    a, b = t[..., :half].astype(jnp.float32), t[..., half:].astype(jnp.float32)
    return jnp.concatenate([a * cos - b * sin, b * cos + a * sin], -1).astype(jnp.bfloat16)


def matmul(a, w):
    return jnp.dot(a, w, preferred_element_type=jnp.float32).astype(jnp.bfloat16)


def einsum(form, a, b):
    return jnp.einsum(form, a.astype(jnp.float32), b.astype(jnp.float32))


def attention(q, k, v):
    scores = einsum("tgsd,ugd->gstu", q, k) * q.shape[-1] ** -0.5
    token = jnp.arange(q.shape[0])
    scores = jnp.where(token[:, None] >= token, scores, -jnp.inf)
    weights = jax.nn.softmax(scores, -1).astype(jnp.bfloat16)
    return einsum("gstu,ugd->tgsd", weights, v).astype(jnp.bfloat16)


def forward(x, gain, wq, wk, wv, wo):
    rows = x.shape[0]
    a, place = normed(x, gain), jnp.arange(rows)
    k = turned(matmul(a, wk).reshape(rows, -1, HEAD), place, THETA)
    q = turned(matmul(a, wq).reshape(rows, -1, HEAD), place, THETA).reshape(rows, k.shape[1], -1, HEAD)
    v = matmul(a, wv).reshape(rows, -1, HEAD)
    seen = attention(q, k, v).reshape(rows, -1)
    return (x.astype(jnp.float32) + jnp.dot(seen, wo, preferred_element_type=jnp.float32)).astype(jnp.bfloat16)


def reference(x, dy, gain, wq, wk, wv, wo):
    _, back = jax.vjp(forward, x, gain.astype(jnp.float32), wq, wk, wv, wo)
    by_x, by_gain, *by_weights = back(dy)
    return (by_x, by_gain[None], *by_weights)
```

```python
import functools

import jax
import jax.numpy as jnp
import numpy as np
from jax import lax
from jax.experimental import pallas as pl
from jax.experimental.pallas import tpu as pltpu
from jax.sharding import PartitionSpec as P

HEAD = 256
HALF = HEAD // 2
THETA = 10000
LOG2E = 1.4426950408889634
NEG = -1e30
HIDDEN = 2 * NEG
ROWS = 2048
D = 2304
OWN = 512
CH = 128
NCH = OWN // CH
SCALE = HEAD**-0.5
E2 = SCALE * LOG2E
BF = jnp.bfloat16
F32 = jnp.float32
ANY = pl.BlockSpec(memory_space=pl.ANY)
VM = pl.BlockSpec(memory_space=pltpu.VMEM)


def _dot(a, b, ca, cb):
    return lax.dot_general(a, b, (((ca,), (cb,)), ((), ())), preferred_element_type=F32)


def _tables():
    freq = THETA ** (-np.arange(HALF) / HALF)
    low = np.arange(CH)[:, None] * freq
    high = (np.arange(ROWS // CH) * CH)[:, None] * freq
    return [np.asarray(f(t), np.float32) for t in (low, high) for f in (np.cos, np.sin)]


def _angles(cl, sl, ch, sh, block):
    c, s = ch[pl.ds(block, 1), :], sh[pl.ds(block, 1), :]
    return cl[...] * c - sl[...] * s, sl[...] * c + cl[...] * s


def _ids():
    t = lax.axis_index("tp")
    chip = lax.div(t, 2)
    core = t - 2 * chip
    return t, chip, core, 2 * (1 - chip) + core, 2 * chip + 1 - core


def _rows(block, n, size=CH):
    return pl.ds(pl.multiple_of(block * OWN + n * size, size), size)


def _barrier(peers):
    barrier = pltpu.get_barrier_semaphore()
    for p in peers:
        pl.semaphore_signal(barrier, inc=1, device_id={"tp": p}, device_id_type=pl.DeviceIdType.MESH)
    pl.semaphore_wait(barrier, len(peers))


def _send(src, dst, send, recv, to):
    return pltpu.make_async_remote_copy(src_ref=src, dst_ref=dst, send_sem=send, recv_sem=recv, device_id={"tp": to},
                                        device_id_type=pl.DeviceIdType.MESH)


def _gather_kernel(x_ref, dy_ref, gain_ref, wq_ref, wk_ref, wv_ref, wo_ref, cl, sl, ch, sh,
                   a_out, dy_out, q_out, k_out, v_out, seen_out, do_out, stat_out,
                   x_s, a_s, dy_s, w_s, wo_s, q_s, k_s, v_s, vt_s, seen_s, seent_s, do_s, top_s, mix_s,
                   send_sem, recv_sem, load_sem, store_sem):
    t, chip, core, over, beside = _ids()
    across = 2 * (1 - chip) + 1 - core

    def piece(kind, way, n, block, to):
        buf = a_s if kind == 0 else dy_s
        return _send(buf.at[_rows(block, n), :], buf.at[_rows(block, n), :], send_sem.at[kind, way, n], recv_sem.at[kind, way, n], to)

    loads = [pltpu.make_async_copy(src, dst, load_sem.at[i]) for i, (src, dst) in enumerate([
        (x_ref, x_s), (dy_ref, dy_s.at[_rows(t, 0, OWN), :]), (wq_ref, w_s.at[:, pl.ds(0, 512)]), (wk_ref, w_s.at[:, pl.ds(512, 256)]),
        (wv_ref, w_s.at[:, pl.ds(768, 256)]), (wo_ref, wo_s)])]
    for c in loads:
        c.start()
    _barrier([over, beside])
    vt_s[HEAD:, :] = jnp.ones((8, ROWS), BF)
    loads[0].wait()

    def norm(n, _):
        wide = x_s[pl.ds(pl.multiple_of(n * CH, CH), CH), :].astype(F32)
        scale = lax.rsqrt(jnp.mean(wide * wide, -1, keepdims=True) + 1e-6)
        a_s[_rows(t, n), :] = (wide * scale * gain_ref[...]).astype(BF)

        @pl.when(n >= 1)
        def _():
            piece(0, 0, n - 1, t, over).start()
            piece(0, 1, n - 1, t, beside).start()

    lax.fori_loop(0, NCH, norm, None)
    loads[1].wait()
    piece(0, 0, NCH - 1, t, over).start()
    piece(0, 1, NCH - 1, t, beside).start()
    for n in range(NCH):
        piece(1, 0, n, t, over).start()
        piece(1, 1, n, t, beside).start()
    for i in range(2, 6):
        loads[i].wait()

    def turn(u, cos, sin):
        a, b = u[:, :HALF].astype(BF).astype(F32), u[:, HALF:].astype(BF).astype(F32)
        return jnp.concatenate([a * cos - b * sin, b * cos + a * sin], -1).astype(BF)

    def project(block, n):
        rows = _rows(block, n)
        cos, sin = _angles(cl, sl, ch, sh, block * NCH + n)
        u = jnp.dot(a_s[rows, :], w_s[...], preferred_element_type=F32)
        q_s[0, rows, :] = turn(u[:, :256], cos, sin)
        q_s[1, rows, :] = turn(u[:, 256:512], cos, sin)
        k_s[rows, :] = turn(u[:, 512:768], cos, sin)
        v = u[:, 768:].astype(BF)
        v_s[rows, :] = v
        vt_s[:HEAD, rows] = v.T

    def grad_seen(block, n):
        rows = _rows(block, n)
        u = _dot(dy_s[rows, :], wo_s[...], 1, 1)
        do_s[0, rows, :] = u[:, :256].astype(BF)
        do_s[1, rows, :] = u[:, 256:].astype(BF)

    def deltas(block, n):
        rows = _rows(block, n)
        for h in range(2):
            prod = do_s[h, rows, :].astype(F32) * seen_s[h, rows, :].astype(F32)
            stat_out[2 + h : 3 + h, rows] = prod.T.sum(axis=0, keepdims=True)

    lax.fori_loop(0, NCH, lambda n, _: project(t, n), None)

    def other(n, _):
        piece(0, 1, n, beside, beside).wait_recv()
        project(beside, n)

    lax.fori_loop(0, NCH, other, None)

    def arrive(n, _):
        piece(0, 0, n, over, over).wait_recv()
        piece(0, 2, n, over, beside).start()
        project(over, n)
        piece(0, 2, n, across, beside).wait_recv()
        project(across, n)

    lax.fori_loop(0, NCH, arrive, None)
    stores = [pltpu.make_async_copy(src, dst, store_sem.at[i]) for i, (src, dst) in enumerate([
        (a_s, a_out), (q_s, q_out), (k_s, k_out), (v_s, v_out), (seent_s, seen_out)])]
    for c in stores[:4]:
        c.start()

    def dy_store(block, n, i):
        return [pltpu.make_async_copy(dy_s.at[_rows(block, n), :], dy_out.at[_rows(block, n), :], store_sem.at[5 + 2 * i]),
                pltpu.make_async_copy(do_s.at[:, _rows(block, n), :], do_out.at[:, _rows(block, n), :], store_sem.at[6 + 2 * i])]

    def near(n, _):
        grad_seen(t, n)
        piece(1, 1, n, beside, beside).wait_recv()
        grad_seen(beside, n)
        for c in dy_store(t, n, n) + dy_store(beside, n, NCH + n):
            c.start()

    lax.fori_loop(0, NCH, near, None)

    def queries(i, _):
        rows = _rows(i, 0, OWN)
        top_s[...] = jnp.full((2, OWN), NEG, F32)
        mix_s[...] = jnp.zeros((2, HEAD + 8, OWN), F32)

        def block(j, masked):
            here = _rows(j, 0, OWN)
            keys = k_s[here, :]
            scores = [_dot(keys, q_s[h, rows, :], 1, 1) for h in range(2)]
            weights, keeps = [], []
            for h in range(2):
                s = scores[h]
                if masked:
                    s = jnp.where(lax.broadcasted_iota(jnp.int32, (OWN, OWN), 1) >= lax.broadcasted_iota(jnp.int32, (OWN, OWN), 0), s, HIDDEN)
                old = top_s[h : h + 1, :]
                top = jnp.maximum(old, s.max(axis=0, keepdims=True))
                top_s[h : h + 1, :] = top
                weights.append(jnp.exp2((s - top) * E2).astype(BF))
                keeps.append(jnp.exp2((old - top) * E2))
            for h in range(2):
                mix_s[h] = mix_s[h] * keeps[h] + _dot(vt_s[:, here], weights[h], 1, 0)

        lax.fori_loop(0, i, lambda j, _: block(j, False), None)
        block(i, True)
        for h in range(2):
            total = mix_s[h, HEAD : HEAD + 1, :]
            out = mix_s[h, :HEAD, :] * (1 / total)
            seent_s[pl.ds(h * HEAD, HEAD), rows] = out.astype(BF)
            seen_s[h, rows, :] = out.T.astype(BF)
            stat_out[h : h + 1, rows] = top_s[h : h + 1, :] * E2 + jnp.log2(total)

    lax.fori_loop(0, ROWS // OWN, queries, None)
    stores[4].start()

    def near_deltas(n, _):
        deltas(t, n)
        deltas(beside, n)

    lax.fori_loop(0, NCH, near_deltas, None)

    def dy_arrive(n, _):
        piece(1, 0, n, over, over).wait_recv()
        piece(1, 2, n, over, beside).start()
        grad_seen(over, n)
        deltas(over, n)
        piece(1, 2, n, across, beside).wait_recv()
        grad_seen(across, n)
        deltas(across, n)
        for c in dy_store(over, n, 2 * NCH + n) + dy_store(across, n, 3 * NCH + n):
            c.start()

    lax.fori_loop(0, NCH, dy_arrive, None)
    for c in stores:
        c.wait()

    def finish(n, _):
        for i, block in enumerate((t, beside, over, across)):
            for c in dy_store(block, n, i * NCH + n):
                c.wait()
        for kind in range(2):
            piece(kind, 0, n, t, over).wait_send()
            piece(kind, 1, n, t, beside).wait_send()
            piece(kind, 2, n, over, beside).wait_send()

    lax.fori_loop(0, NCH, finish, None)


def _gather(x, dy, gain, wq, wk, wv, wo):
    tables = [jnp.asarray(u) for u in _tables()]
    sds = jax.ShapeDtypeStruct
    heads = sds((2, ROWS, HEAD), BF)
    one = sds((ROWS, HEAD), BF)
    whole = sds((ROWS, D), BF)
    vm = lambda s, d=BF: pltpu.VMEM(s, d)
    return pl.pallas_call(
        _gather_kernel,
        out_shape=[whole, whole, heads, one, one, sds((2 * HEAD, ROWS), BF), heads, sds((8, ROWS), F32)],
        in_specs=[ANY, ANY, VM, ANY, ANY, ANY, ANY, VM, VM, VM, VM],
        out_specs=[ANY] * 7 + [VM],
        scratch_shapes=[vm((OWN, D)), vm((ROWS, D)), vm((ROWS, D)), vm((D, 1024)), vm((512, D)), vm((2, ROWS, HEAD)), vm((ROWS, HEAD)),
                        vm((ROWS, HEAD)), vm((HEAD + 8, ROWS)), vm((2, ROWS, HEAD)), vm((2 * HEAD, ROWS)), vm((2, ROWS, HEAD)), vm((2, OWN), F32),
                        vm((2, HEAD + 8, OWN), F32), pltpu.SemaphoreType.DMA((2, 3, NCH)), pltpu.SemaphoreType.DMA((2, 3, NCH)),
                        pltpu.SemaphoreType.DMA((6,)), pltpu.SemaphoreType.DMA((5 + 8 * NCH,))],
        compiler_params=pltpu.CompilerParams(collective_id=0, has_side_effects=True, vmem_limit_bytes=67000000),
        name="gather",
    )(x, dy, gain.astype(F32)[None], wq, wk, wv, wo, *tables)


PIECE = 256
TILE = 256


def _grads_kernel(x_ref, dy_ref, gain_ref, wq_ref, wk_ref, wv_ref, cl, sl, ch, sh, a_ref, dyf_ref, q_ref, k_ref, v_ref, seen_ref, do_ref, stat,
                  dx_out, dgain_out, dwq_out, dwk_out, dwv_out, dwo_out,
                  x_s, dy_s, w_s, q_s, k_s, v_s, seen_s, do_s, dq_s, dk_s, dv_s, g_s, near_send, near_recv, over_recv, loc_send,
                  loc_recv, own_s, a_t, dw_t, dwo_t, dg_s,
                  load_sem, near_sem, over_send_sem, over_recv_sem, loc_sem, gain_send_sem, gain_recv_sem, at_sem, dyt_sem, dw_sem, dwo_sem, out_sem):
    t, chip, core, over, beside = _ids()
    across = 2 * (1 - chip) + 1 - core
    pairs = [(k_ref, k_s), (v_ref, v_s), (q_ref, q_s), (do_ref, do_s), (wq_ref, w_s.at[:, pl.ds(0, 512)]), (wk_ref, w_s.at[:, pl.ds(512, 256)]),
             (wv_ref, w_s.at[:, pl.ds(768, 256)]), (seen_ref, seen_s), (x_ref, x_s), (dy_ref, dy_s)]
    loads = [pltpu.make_async_copy(src, dst, load_sem.at[i]) for i, (src, dst) in enumerate(pairs)]
    for c in loads:
        c.start()

    def a_tile(i, slot):
        return pltpu.make_async_copy(a_ref.at[:, pl.ds(pl.multiple_of(i * TILE, TILE), TILE)], a_t.at[slot], at_sem.at[slot])

    def dy_tile(i, slot):
        return pltpu.make_async_copy(dyf_ref.at[:, pl.ds(pl.multiple_of(i * TILE, TILE), TILE)], q_s.at[slot], dyt_sem.at[slot])

    a_tile(0, 0).start()
    dq_s[...] = jnp.zeros_like(dq_s)
    dk_s[...] = jnp.zeros_like(dk_s)
    dv_s[...] = jnp.zeros_like(dv_s)
    _barrier([over, beside, across])
    for c in loads[:4]:
        c.wait()

    def pair(i, j, masked):
        cols, here = _rows(i, 0, OWN), _rows(j, 0, OWN)
        keys, values = k_s[here, :], v_s[here, :]
        qs = [q_s[h, cols, :] for h in range(2)]
        dos = [do_s[h, cols, :] for h in range(2)]
        scores = [_dot(keys, qs[h], 1, 1) for h in range(2)]
        dps = [_dot(values, dos[h], 1, 1) for h in range(2)]
        ps, dss = [], []
        for h in range(2):
            p = jnp.exp2(scores[h] * E2 - stat[h : h + 1, cols])
            if masked:
                p = jnp.where(lax.broadcasted_iota(jnp.int32, (OWN, OWN), 1) >= lax.broadcasted_iota(jnp.int32, (OWN, OWN), 0), p, 0.0)
            dss.append((p * (dps[h] - stat[2 + h : 3 + h, cols])).astype(BF))
            ps.append(p.astype(BF))
        dv_s[here, :] += _dot(jnp.concatenate(ps, 1), jnp.concatenate(dos, 0), 1, 0)
        dk_s[here, :] += _dot(jnp.concatenate(dss, 1), jnp.concatenate(qs, 0), 1, 0)
        turned_keys = keys.T
        for h in range(2):
            dq_s[h, :, cols] += _dot(turned_keys, dss[h], 1, 0)

    def unturn(g, cos, sin):
        g = g.astype(BF).astype(F32)
        a, b = g[:, :HALF], g[:, HALF:]
        return jnp.concatenate([a * cos + b * sin, b * cos - a * sin], -1).astype(BF)

    def done(block, n):
        rows = _rows(block, n)
        cos, sin = _angles(cl, sl, ch, sh, block * NCH + n)
        for h in range(2):
            g_s[rows, pl.ds(h * HEAD, HEAD)] = unturn((dq_s[h, :, rows] * SCALE).T, cos, sin)
        g_s[rows, pl.ds(512, HEAD)] = unturn(dk_s[rows, :] * SCALE, cos, sin)
        g_s[rows, pl.ds(768, HEAD)] = dv_s[rows, :].astype(BF)

    def term(block, half):
        return _dot(g_s[_rows(block, half, PIECE), :], w_s[...], 1, 1)

    def near(u):
        return _send(near_send.at[u], near_recv.at[u], near_sem.at[0, u], near_sem.at[1, u], beside)

    def to_owner(u, n, block):
        rows = pl.ds(n * CH, CH)
        return _send(near_send.at[u, rows, :], over_recv.at[pl.ds(pl.multiple_of(core * PIECE + n * CH, CH), CH), :], over_send_sem.at[u, n],
                     over_recv_sem.at[core, n], block)

    def from_over(half, n):
        rows = over_recv.at[pl.ds(half * PIECE + n * CH, CH), :]
        return _send(rows, rows, over_send_sem.at[0, n], over_recv_sem.at[half, n], over)

    def local():
        return _send(loc_send, loc_recv, loc_sem.at[0], loc_sem.at[1], beside)

    def step(u, _):
        block = jnp.where(chip == 1, u, 3 - u)
        pair(block, block, True)

        def others(w, _):
            pair(jnp.where(chip == 1, w, 3 - u), jnp.where(chip == 1, u, 3 - w), False)

        lax.fori_loop(u + 1, 4, others, None)
        lax.fori_loop(0, NCH, lambda n, _: done(block, n), None)

        @pl.when(u == 0)
        def _():
            for c in loads[4:7]:
                c.wait()

        @pl.when(u < 2)
        def _():
            near_send[u] = term(block, 1 - core).astype(BF)
            near(u).start()
            mine = term(block, core)
            near(u).wait()
            near_send[u] = (mine + near_recv[u].astype(F32)).astype(BF)
            for n in range(PIECE // CH):
                to_owner(u, n, block).start()

        @pl.when((u >= 2) & (block == t))
        def _():
            for half in range(2):
                own_s[pl.ds(half * PIECE, PIECE), :] = term(block, half)

        @pl.when((u >= 2) & (block != t))
        def _():
            for half in range(2):
                loc_send[pl.ds(half * PIECE, PIECE), :] = term(block, half).astype(BF)
            local().start()

    lax.fori_loop(0, 4, step, None)

    dy_t = q_s
    dy_tile(0, 0).start()

    def dw_store(i, slot):
        rows = pl.ds(pl.multiple_of(i * TILE, TILE), TILE)
        return [pltpu.make_async_copy(dw_t.at[slot, :, pl.ds(at, out.shape[1])], out.at[rows, :], dw_sem.at[slot, m])
                for m, (at, out) in enumerate([(0, dwq_out), (512, dwk_out), (768, dwv_out)])]

    def dw(i, _):
        slot = lax.rem(i, 2)

        @pl.when(i + 1 < D // TILE)
        def _():
            a_tile(i + 1, 1 - slot).start()

        a_tile(i, slot).wait()

        @pl.when(i >= 2)
        def _():
            for c in dw_store(i - 2, slot):
                c.wait()

        dw_t[slot] = _dot(a_t[slot], g_s[...], 0, 0).astype(BF)
        for c in dw_store(i, slot):
            c.start()

    lax.fori_loop(0, D // TILE, dw, None)
    loads[7].wait()

    def dwo_store(i, slot):
        return pltpu.make_async_copy(dwo_t.at[slot], dwo_out.at[:, pl.ds(pl.multiple_of(i * TILE, TILE), TILE)], dwo_sem.at[slot])

    def dwo(i, _):
        slot = lax.rem(i, 2)

        @pl.when(i + 1 < D // TILE)
        def _():
            dy_tile(i + 1, 1 - slot).start()

        dy_tile(i, slot).wait()

        @pl.when(i >= 2)
        def _():
            dwo_store(i - 2, slot).wait()

        dwo_t[slot] = _dot(seen_s[...], dy_t[slot], 1, 0).astype(BF)
        dwo_store(i, slot).start()

    lax.fori_loop(0, D // TILE, dwo, None)
    for i in range(D // TILE - 2, D // TILE):
        for c in dw_store(i, i % 2) + [dwo_store(i, i % 2)]:
            c.wait()

    loads[8].wait()
    loads[9].wait()
    local().wait()
    dg_s[3] = jnp.zeros((1, D), F32)
    dx_store = lambda at: pltpu.make_async_copy(x_s.at[pl.ds(at, CH), :], dx_out.at[pl.ds(at, CH), :], out_sem.at[at // CH])
    for n in range(PIECE // CH):
        for half in range(2):
            from_over(half, n).wait_recv()
            at = half * PIECE + n * CH
            rows = pl.ds(at, CH)
            da = own_s[rows, :] + loc_recv[rows, :].astype(F32) + over_recv[rows, :].astype(F32)
            wide = x_s[rows, :].astype(F32)
            scale = lax.rsqrt(jnp.mean(wide * wide, -1, keepdims=True) + 1e-6)
            dg_s[3] += jnp.sum(da * wide * scale, 0, keepdims=True)
            da = da * gain_ref[...]
            pull = jnp.sum(da * wide, -1, keepdims=True) * scale * scale * scale * (-1 / D)
            x_s[rows, :] = (da * scale + pull * wide + dy_s[rows, :].astype(F32)).astype(BF)
            dx_store(at).start()

    def gains(m):
        return _send(dg_s.at[3], dg_s.at[m], gain_send_sem.at[m], gain_recv_sem.at[m], (over, beside, across)[m])

    for m in range(3):
        gains(m).start()
    for m in range(3):
        gains(m).wait()
    dgain_out[...] = dg_s[3] + dg_s[0] + dg_s[1] + dg_s[2]
    for u in range(2):
        for n in range(PIECE // CH):
            to_owner(u, n, jnp.where(chip == 1, u, 3 - u)).wait_send()
    for at in range(0, OWN, CH):
        dx_store(at).wait()


def _grads(x, dy, gain, wq, wk, wv, a, dyf, q, k, v, seen, do, stat):
    tables = [jnp.asarray(u) for u in _tables()]
    sds = jax.ShapeDtypeStruct
    vm = lambda s, d=BF: pltpu.VMEM(s, d)
    dma = lambda *s: pltpu.SemaphoreType.DMA(s)
    return pl.pallas_call(
        _grads_kernel,
        out_shape=[sds((OWN, D), BF), sds((1, D), F32), sds((D, 512), BF), sds((D, 256), BF), sds((D, 256), BF), sds((512, D), BF)],
        in_specs=[ANY, ANY, VM, ANY, ANY, ANY, VM, VM, VM, VM] + [ANY] * 7 + [VM],
        out_specs=[ANY, VM, ANY, ANY, ANY, ANY],
        scratch_shapes=[
            vm((OWN, D)), vm((OWN, D)), vm((D, 1024)), vm((2, ROWS, HEAD)), vm((ROWS, HEAD)), vm((ROWS, HEAD)), vm((2 * HEAD, ROWS)),
            vm((2, ROWS, HEAD)), vm((2, HEAD, ROWS), F32), vm((ROWS, HEAD), F32), vm((ROWS, HEAD), F32), vm((ROWS, 1024)),
            vm((2, PIECE, D)), vm((2, PIECE, D)), vm((OWN, D)), vm((OWN, D)), vm((OWN, D)), vm((OWN, D), F32),
            vm((2, ROWS, TILE)), vm((2, TILE, 1024)), vm((2, 512, TILE)), vm((4, 1, D), F32),
            dma(10), dma(2, 2), dma(2, 2), dma(2, 2), dma(2), dma(3), dma(3), dma(2), dma(2), dma(2, 3), dma(2), dma(NCH)],
        compiler_params=pltpu.CompilerParams(collective_id=1, has_side_effects=True, vmem_limit_bytes=67000000),
        name="grads",
    )(x, dy, gain.astype(F32)[None], wq, wk, wv, *tables, a, dyf, q, k, v, seen, do, stat)


def solution(mesh):
    def step(x, dy, gain, wq, wk, wv, wo):
        return tuple(_grads(x, dy, gain, wq, wk, wv, *_gather(x, dy, gain, wq, wk, wv, wo)))

    tokens, columns = P(("dp", "tp"), None), P(None, "tp")
    return jax.shard_map(
        step,
        mesh=mesh,
        in_specs=(tokens, tokens, P(None), columns, columns, columns, P("tp", None)),
        out_specs=(tokens, P("dp", None), P("dp", "tp"), P("dp", "tp"), P("dp", "tp"), P(("dp", "tp"), None)),
        check_vma=False,
    )
```

```python
import functools

import jax
import jax.numpy as jnp
import numpy as np
from jax import lax
from jax.experimental import pallas as pl
from jax.experimental.pallas import tpu as pltpu
from jax.sharding import PartitionSpec as P

HEAD = 256
HALF = HEAD // 2
THETA = 10000
LOG2E = 1.4426950408889634
NEG = -1e30
HIDDEN = 2 * NEG
ROWS = 2048
D = 2304
OWN = 512
CH = 128
NCH = OWN // CH
SCALE = HEAD**-0.5
E2 = SCALE * LOG2E
BF = jnp.bfloat16
F32 = jnp.float32
ANY = pl.BlockSpec(memory_space=pl.ANY)
VM = pl.BlockSpec(memory_space=pltpu.VMEM)


def _dot(a, b, ca, cb):
    return lax.dot_general(a, b, (((ca,), (cb,)), ((), ())), preferred_element_type=F32)


def _tables():
    freq = THETA ** (-np.arange(HALF) / HALF)
    low = np.arange(CH)[:, None] * freq
    high = (np.arange(ROWS // CH) * CH)[:, None] * freq
    return [np.asarray(f(t), np.float32) for t in (low, high) for f in (np.cos, np.sin)]


def _angles(cl, sl, ch, sh, block):
    c, s = ch[pl.ds(block, 1), :], sh[pl.ds(block, 1), :]
    return cl[...] * c - sl[...] * s, sl[...] * c + cl[...] * s


def _ids():
    t = lax.axis_index("tp")
    chip = lax.div(t, 2)
    core = t - 2 * chip
    return t, chip, core, 2 * (1 - chip) + core, 2 * chip + 1 - core


def _rows(block, n, size=CH):
    return pl.ds(pl.multiple_of(block * OWN + n * size, size), size)


def _barrier(peers):
    barrier = pltpu.get_barrier_semaphore()
    for p in peers:
        pl.semaphore_signal(barrier, inc=1, device_id={"tp": p}, device_id_type=pl.DeviceIdType.MESH)
    pl.semaphore_wait(barrier, len(peers))


def _send(src, dst, send, recv, to):
    return pltpu.make_async_remote_copy(src_ref=src, dst_ref=dst, send_sem=send, recv_sem=recv, device_id={"tp": to},
                                        device_id_type=pl.DeviceIdType.MESH)


PIECE = 256
TILE = 256


def _kernel(x_ref, dy_ref, gain_ref, wq_ref, wk_ref, wv_ref, wo_ref, cl, sl, ch, sh,
            dx_out, dgain_out, dwq_out, dwk_out, dwv_out, dwo_out, a_out,
            x_s, a_s, dy_s, w_s, wo_s, q_s, k_s, v_s, seent_s, do_s, top_s, mix_s, stat, dq_s, dk_s, dv_s, g_s, dw_t, dwo_t, dg_s,
            send_sem, recv_sem, load_sem, a_sem, near_sem, over_send_sem, over_recv_sem, loc_sem, gain_send_sem, gain_recv_sem,
            at_sem, dw_sem, dwo_sem, out_sem, ready_sem):
    t, chip, core, over, beside = _ids()
    across = 2 * (1 - chip) + 1 - core
    peers = (over, beside, across)

    def state(way, n, block, to):
        at = a_s.at[_rows(block, n), :]
        return _send(at, at, send_sem.at[0, way, n], recv_sem.at[0, way, n], to)

    def dy_own(n, block):
        at = dy_s.at[_rows(block, n), :]
        return _send(at, at, send_sem.at[1, 1, n], recv_sem.at[1, 1, n], beside)

    def dy_piece(way, n, of_chip, half, to):
        block = 2 * of_chip + 1 - lax.div(n, 2)
        at = dy_s.at[pl.ds(pl.multiple_of(block * OWN + half * PIECE + lax.rem(n, 2) * CH, CH), CH), :]
        return _send(at, at, send_sem.at[1, way, n], recv_sem.at[1, way, n], to)

    loads = [pltpu.make_async_copy(src, dst, load_sem.at[i]) for i, (src, dst) in enumerate([
        (x_ref, x_s), (dy_ref, dy_s.at[_rows(t, 0, OWN), :]), (wq_ref, w_s.at[:, pl.ds(0, 512)]), (wk_ref, w_s.at[:, pl.ds(512, 256)]),
        (wv_ref, w_s.at[:, pl.ds(768, 256)]), (wo_ref, wo_s)])]
    for c in loads:
        c.start()
    _barrier(peers)
    loads[0].wait()

    def norm(n, _):
        wide = x_s[pl.ds(pl.multiple_of(n * CH, CH), CH), :].astype(F32)
        scale = lax.rsqrt(jnp.mean(wide * wide, -1, keepdims=True) + 1e-6)
        a_s[_rows(t, n), :] = (wide * scale * gain_ref[...]).astype(BF)

        @pl.when(n >= 1)
        def _():
            state(0, n - 1, t, over).start()
            state(1, n - 1, t, beside).start()

    lax.fori_loop(0, NCH, norm, None)
    loads[1].wait()
    state(0, NCH - 1, t, over).start()
    state(1, NCH - 1, t, beside).start()
    for n in range(NCH):
        dy_own(n, t).start()
    for i in range(2, 6):
        loads[i].wait()

    def turn(u, cos, sin):
        a, b = u[:, :HALF].astype(BF).astype(F32), u[:, HALF:].astype(BF).astype(F32)
        return jnp.concatenate([a * cos - b * sin, b * cos + a * sin], -1).astype(BF)

    def unturn(g, cos, sin):
        g = g.astype(BF).astype(F32)
        a, b = g[:, :HALF], g[:, HALF:]
        return jnp.concatenate([a * cos + b * sin, b * cos - a * sin], -1).astype(BF)

    def project(block, n):
        rows = _rows(block, n)
        cos, sin = _angles(cl, sl, ch, sh, block * NCH + n)
        u = jnp.dot(a_s[rows, :], w_s[...], preferred_element_type=F32)
        q_s[0, rows, :] = turn(u[:, :256], cos, sin)
        q_s[1, rows, :] = turn(u[:, 256:512], cos, sin)
        k_s[rows, :] = turn(u[:, 512:768], cos, sin)
        v_s[rows, :] = u[:, 768:].astype(BF)

    def grad_seen(block):
        rows = _rows(block, 0, OWN)
        u = _dot(dy_s[rows, :], wo_s[...], 1, 1)
        do_s[0, rows, :] = u[:, :256].astype(BF)
        do_s[1, rows, :] = u[:, 256:].astype(BF)

    def deltas(block):
        def some(n, _):
            rows = _rows(block, n)
            for h in range(2):
                prod = do_s[h, rows, :].astype(F32) * g_s[rows, pl.ds(h * HEAD, HEAD)].astype(F32)
                stat[2 + h : 3 + h, rows] = prod.T.sum(axis=0, keepdims=True)

        lax.fori_loop(0, NCH, some, None)

    lax.fori_loop(0, NCH, lambda n, _: project(t, n), None)
    for n in range(NCH):
        dy_own(n, beside).wait_recv()
    for n in range(NCH):
        dy_piece(0, n, chip, core, over).start()

    def other(n, _):
        state(1, n, beside, beside).wait_recv()
        project(beside, n)

    lax.fori_loop(0, NCH, other, None)
    lax.fori_loop(0, 2, lambda m, _: grad_seen(2 * chip + m), None)
    dk_s[...] = jnp.zeros_like(dk_s)
    dv_s[...] = jnp.zeros_like(dv_s)

    def arrive(n, _):
        state(0, n, over, over).wait_recv()
        state(2, n, over, beside).start()
        project(over, n)
        state(2, n, across, beside).wait_recv()
        project(across, n)

    lax.fori_loop(0, NCH, arrive, None)
    a_store = pltpu.make_async_copy(a_s, a_out, a_sem)
    a_store.start()

    def hide(s, other):
        ok = lax.broadcasted_iota(jnp.int32, (OWN, OWN), 1) >= lax.broadcasted_iota(jnp.int32, (OWN, OWN), 0)
        return jnp.where(ok, s, other)

    def queries(i, _):
        rows = _rows(i, 0, OWN)
        top_s[...] = jnp.full((2, OWN), NEG, F32)
        mix_s[...] = jnp.zeros((2, HEAD + 8, OWN), F32)

        def block(j, masked):
            here = _rows(j, 0, OWN)
            keys = k_s[here, :]
            scores = [_dot(keys, q_s[h, rows, :], 1, 1) for h in range(2)]
            values = jnp.concatenate([v_s[here, :].T, jnp.ones((8, OWN), BF)], 0)
            weights, keeps = [], []
            for h in range(2):
                s = hide(scores[h], HIDDEN) if masked else scores[h]
                old = top_s[h : h + 1, :]
                top = jnp.maximum(old, s.max(axis=0, keepdims=True))
                top_s[h : h + 1, :] = top
                weights.append(jnp.exp2((s - top) * E2).astype(BF))
                keeps.append(jnp.exp2((old - top) * E2))
            for h in range(2):
                mix_s[h] = mix_s[h] * keeps[h] + _dot(values, weights[h], 1, 0)

        lax.fori_loop(0, i, lambda j, _: block(j, False), None)
        block(i, True)
        for h in range(2):
            total = mix_s[h, HEAD : HEAD + 1, :]
            out = mix_s[h, :HEAD, :] * (1 / total)
            seent_s[pl.ds(h * HEAD, HEAD), rows] = out.astype(BF)
            g_s[rows, pl.ds(h * HEAD, HEAD)] = out.T.astype(BF)
            stat[h : h + 1, rows] = top_s[h : h + 1, :] * E2 + jnp.log2(total)

    lax.fori_loop(0, ROWS // OWN, queries, None)

    def sent(n, _):
        state(0, n, t, over).wait_send()
        state(1, n, t, beside).wait_send()
        state(2, n, over, beside).wait_send()

    lax.fori_loop(0, NCH, sent, None)
    a_store.wait()
    for p in peers:
        pl.semaphore_signal(ready_sem, inc=1, device_id={"tp": p}, device_id_type=pl.DeviceIdType.MESH)
    near_at = lambda u: a_s.at[pl.ds(u * PIECE, PIECE), :]
    near_in = lambda u: a_s.at[pl.ds(OWN + u * PIECE, PIECE), :]
    over_at = 2 * OWN
    loc_in = a_s.at[pl.ds(3 * OWN, OWN), :]

    def pair(i, j, masked):
        cols, here = _rows(i, 0, OWN), _rows(j, 0, OWN)
        keys, values = k_s[here, :], v_s[here, :]
        qs = [q_s[h, cols, :] for h in range(2)]
        dos = [do_s[h, cols, :] for h in range(2)]
        scores = [_dot(keys, qs[h], 1, 1) for h in range(2)]
        dps = [_dot(values, dos[h], 1, 1) for h in range(2)]
        ps, dss = [], []
        for h in range(2):
            p = jnp.exp2(scores[h] * E2 - stat[h : h + 1, cols])
            p = hide(p, 0.0) if masked else p
            dss.append((p * (dps[h] - stat[2 + h : 3 + h, cols])).astype(BF))
            ps.append(p.astype(BF))
        dv_s[here, :] += _dot(jnp.concatenate(ps, 1), jnp.concatenate(dos, 0), 1, 0)
        dk_s[here, :] += _dot(jnp.concatenate(dss, 1), jnp.concatenate(qs, 0), 1, 0)
        turned_keys = keys.T
        for h in range(2):
            dq_s[h] += _dot(turned_keys, dss[h], 1, 0)

    def queries_back(i):
        deltas(i)
        dq_s[...] = jnp.zeros_like(dq_s)
        lax.fori_loop(0, i, lambda j, _: pair(i, j, False), None)
        pair(i, i, True)
        for n in range(NCH):
            rows = _rows(i, n)
            cos, sin = _angles(cl, sl, ch, sh, i * NCH + n)
            for h in range(2):
                g_s[rows, pl.ds(h * HEAD, HEAD)] = unturn((dq_s[h, :, n * CH : (n + 1) * CH] * SCALE).T, cos, sin)

    def keys_done(block):
        def some(n, _):
            rows = _rows(block, n)
            cos, sin = _angles(cl, sl, ch, sh, block * NCH + n)
            g_s[rows, pl.ds(512, HEAD)] = unturn(dk_s[rows, :] * SCALE, cos, sin)
            g_s[rows, pl.ds(768, HEAD)] = dv_s[rows, :].astype(BF)

        lax.fori_loop(0, NCH, some, None)

    def term(block, half):
        return _dot(g_s[_rows(block, half, PIECE), :], w_s[...], 1, 1)

    def near(u):
        return _send(near_at(u), near_in(u), near_sem.at[0, u], near_sem.at[1, u], beside)

    def to_owner(u, n):
        return _send(a_s.at[pl.ds(pl.multiple_of(u * PIECE + n * CH, CH), CH), :],
                     a_s.at[pl.ds(pl.multiple_of(over_at + core * PIECE + n * CH, CH), CH), :],
                     over_send_sem.at[u, n], over_recv_sem.at[core, n], 2 * (1 - chip) + 1 - u)

    def from_over(half, n):
        rows = a_s.at[pl.ds(over_at + half * PIECE + n * CH, CH), :]
        return _send(rows, rows, over_send_sem.at[0, n], over_recv_sem.at[half, n], over)

    def local():
        return _send(x_s, loc_in, loc_sem.at[0], loc_sem.at[1], beside)

    lax.fori_loop(0, 2, lambda m, _: queries_back(2 * chip + m), None)
    pl.semaphore_wait(ready_sem, 3)

    def far(u, _):
        block = 2 * (1 - chip) + 1 - u
        for m in range(2):
            dy_piece(0, 2 * u + m, 1 - chip, core, over).wait_recv()
            dy_piece(2, 2 * u + m, 1 - chip, core, beside).start()
        for m in range(2):
            dy_piece(2, 2 * u + m, 1 - chip, 1 - core, beside).wait_recv()
        grad_seen(block)
        queries_back(block)
        keys_done(block)
        near_at(u)[...] = term(block, 1 - core).astype(BF)
        near(u).start()
        mine = term(block, core)
        near(u).wait()
        near_at(u)[...] = (mine + near_in(u)[...].astype(F32)).astype(BF)
        for n in range(PIECE // CH):
            to_owner(u, n).start()

    lax.fori_loop(0, 2, far, None)

    def a_tile(i, slot):
        return pltpu.make_async_copy(a_out.at[:, pl.ds(pl.multiple_of(i * TILE, TILE), TILE)], do_s.at[slot], at_sem.at[slot])

    a_tile(0, 0).start()
    lax.fori_loop(0, 2, lambda m, _: keys_done(2 * chip + m), None)
    for half in range(2):
        x_s[pl.ds(half * PIECE, PIECE), :] = term(beside, half).astype(BF)
    local().start()
    own = lambda c, at, size: (dk_s.at[pl.ds(c * OWN + at, size), :] if c < 4 else dv_s.at[pl.ds((c - 4) * OWN + at, size), :] if c < 8
                               else dq_s.at[at // PIECE, pl.ds(at % PIECE, size), pl.ds(0, 256)])
    for half in range(2):
        mine = term(t, half)
        for c in range(D // 256):
            own(c, half * PIECE, PIECE)[...] = mine[:, c * 256 : (c + 1) * 256]

    def dw_store(i, slot):
        rows = pl.ds(pl.multiple_of(i * TILE, TILE), TILE)
        return [pltpu.make_async_copy(dw_t.at[slot, :, pl.ds(at, out.shape[1])], out.at[rows, :], dw_sem.at[slot, m])
                for m, (at, out) in enumerate([(0, dwq_out), (512, dwk_out), (768, dwv_out)])]

    def dw(i, _):
        slot = lax.rem(i, 2)

        @pl.when(i + 1 < D // TILE)
        def _():
            a_tile(i + 1, 1 - slot).start()

        a_tile(i, slot).wait()

        @pl.when(i >= 2)
        def _():
            for c in dw_store(i - 2, slot):
                c.wait()

        dw_t[slot] = _dot(do_s[slot], g_s[...], 0, 0).astype(BF)
        for c in dw_store(i, slot):
            c.start()

    lax.fori_loop(0, D // TILE, dw, None)
    local().wait()
    again = pltpu.make_async_copy(x_ref, x_s, load_sem.at[0])
    again.start()

    def dwo_store(i, slot):
        return pltpu.make_async_copy(dwo_t.at[slot], dwo_out.at[:, pl.ds(pl.multiple_of(i * TILE, TILE), TILE)], dwo_sem.at[slot])

    def dwo(i, _):
        slot = lax.rem(i, 2)

        @pl.when(i >= 2)
        def _():
            dwo_store(i - 2, slot).wait()

        dwo_t[slot] = _dot(seent_s[...], dy_s[:, pl.ds(pl.multiple_of(i * TILE, TILE), TILE)], 1, 0).astype(BF)
        dwo_store(i, slot).start()

    lax.fori_loop(0, D // TILE, dwo, None)
    for i in range(D // TILE - 2, D // TILE):
        for c in dw_store(i, i % 2) + [dwo_store(i, i % 2)]:
            c.wait()

    again.wait()
    dg_s[3] = jnp.zeros((1, D), F32)
    dx_store = lambda at: pltpu.make_async_copy(x_s.at[pl.ds(at, CH), :], dx_out.at[pl.ds(at, CH), :], out_sem.at[at // CH])
    for n in range(PIECE // CH):
        for half in range(2):
            from_over(half, n).wait_recv()
            at = half * PIECE + n * CH
            rows = pl.ds(at, CH)
            mine = jnp.concatenate([own(c, at, CH)[...] for c in range(D // 256)], 1)
            da = mine + a_s[pl.ds(3 * OWN + at, CH), :].astype(F32) + a_s[pl.ds(over_at + at, CH), :].astype(F32)
            wide = x_s[rows, :].astype(F32)
            scale = lax.rsqrt(jnp.mean(wide * wide, -1, keepdims=True) + 1e-6)
            dg_s[3] += jnp.sum(da * wide * scale, 0, keepdims=True)
            da = da * gain_ref[...]
            pull = jnp.sum(da * wide, -1, keepdims=True) * scale * scale * scale * (-1 / D)
            x_s[rows, :] = (da * scale + pull * wide + dy_s[_rows(t, at // CH), :].astype(F32)).astype(BF)
            dx_store(at).start()

    def gains(m):
        return _send(dg_s.at[3], dg_s.at[m], gain_send_sem.at[m], gain_recv_sem.at[m], peers[m])

    for m in range(3):
        gains(m).start()
    for m in range(3):
        gains(m).wait()
    dgain_out[...] = dg_s[3] + dg_s[0] + dg_s[1] + dg_s[2]
    for n in range(NCH):
        dy_own(n, t).wait_send()
        dy_piece(0, n, chip, core, over).wait_send()
        dy_piece(2, n, 1 - chip, core, beside).wait_send()
    for u in range(2):
        for n in range(PIECE // CH):
            to_owner(u, n).wait_send()
    for at in range(0, OWN, CH):
        dx_store(at).wait()


def solution(mesh):
    vm = lambda s, d=BF: pltpu.VMEM(s, d)
    dma = lambda *s: pltpu.SemaphoreType.DMA(s)
    sds = jax.ShapeDtypeStruct

    def step(x, dy, gain, wq, wk, wv, wo):
        tables = [jnp.asarray(u) for u in _tables()]
        return tuple(pl.pallas_call(
            _kernel,
            out_shape=[sds((OWN, D), BF), sds((1, D), F32), sds((D, 512), BF), sds((D, 256), BF), sds((D, 256), BF), sds((512, D), BF),
                       sds((ROWS, D), BF)],
            in_specs=[ANY, ANY, VM, ANY, ANY, ANY, ANY, VM, VM, VM, VM],
            out_specs=[ANY, VM, ANY, ANY, ANY, ANY, ANY],
            scratch_shapes=[
                vm((OWN, D)), vm((ROWS, D)), vm((ROWS, D)), vm((D, 1024)), vm((512, D)), vm((2, ROWS, HEAD)), vm((ROWS, HEAD)),
                vm((ROWS, HEAD)), vm((2 * HEAD, ROWS)), vm((2, ROWS, HEAD)), vm((2, OWN), F32), vm((2, HEAD + 8, OWN), F32),
                vm((8, ROWS), F32), vm((2, HEAD, OWN), F32), vm((ROWS, HEAD), F32), vm((ROWS, HEAD), F32), vm((ROWS, 1024)),
                vm((2, TILE, 1024)), vm((2, 512, TILE)), vm((4, 1, D), F32),
                dma(2, 3, NCH), dma(2, 3, NCH), dma(6), pltpu.SemaphoreType.DMA, dma(2, 2), dma(2, 2), dma(2, 2), dma(2), dma(3), dma(3),
                dma(2), dma(2, 3), dma(2), dma(NCH), pltpu.SemaphoreType.REGULAR],
            compiler_params=pltpu.CompilerParams(collective_id=0, has_side_effects=True, vmem_limit_bytes=67000000),
            name="half",
        )(x, dy, gain.astype(F32)[None], wq, wk, wv, wo, *tables))[:6]

    tokens, columns = P(("dp", "tp"), None), P(None, "tp")
    return jax.shard_map(
        step,
        mesh=mesh,
        in_specs=(tokens, tokens, P(None), columns, columns, columns, P("tp", None)),
        out_specs=(tokens, P("dp", None), P("dp", "tp"), P("dp", "tp"), P("dp", "tp"), P(("dp", "tp"), None)),
        check_vma=False,
    )
```

```python
import functools

import jax
import jax.numpy as jnp
import numpy as np
from jax import lax
from jax.experimental import pallas as pl
from jax.experimental.pallas import tpu as pltpu
from jax.sharding import PartitionSpec as P

HEAD = 256
HALF = HEAD // 2
THETA = 10000
LOG2E = 1.4426950408889634
NEG = -1e30
HIDDEN = 2 * NEG
ROWS = 2048
D = 2304
OWN = 512
CH = 128
NCH = OWN // CH
SCALE = HEAD**-0.5
E2 = SCALE * LOG2E
BF = jnp.bfloat16
F32 = jnp.float32
ANY = pl.BlockSpec(memory_space=pl.ANY)
VM = pl.BlockSpec(memory_space=pltpu.VMEM)


def _dot(a, b, ca, cb):
    return lax.dot_general(a, b, (((ca,), (cb,)), ((), ())), preferred_element_type=F32)


def _tables():
    freq = THETA ** (-np.arange(HALF) / HALF)
    low = np.arange(CH)[:, None] * freq
    high = (np.arange(ROWS // CH) * CH)[:, None] * freq
    return [np.asarray(f(t), np.float32) for t in (low, high) for f in (np.cos, np.sin)]


def _angles(cl, sl, ch, sh, block):
    c, s = ch[pl.ds(block, 1), :], sh[pl.ds(block, 1), :]
    return cl[...] * c - sl[...] * s, sl[...] * c + cl[...] * s


def _ids():
    t = lax.axis_index("tp")
    chip = lax.div(t, 2)
    core = t - 2 * chip
    return t, chip, core, 2 * (1 - chip) + core, 2 * chip + 1 - core


def _rows(block, n, size=CH):
    return pl.ds(pl.multiple_of(block * OWN + n * size, size), size)


def _barrier(peers):
    barrier = pltpu.get_barrier_semaphore()
    for p in peers:
        pl.semaphore_signal(barrier, inc=1, device_id={"tp": p}, device_id_type=pl.DeviceIdType.MESH)
    pl.semaphore_wait(barrier, len(peers))


def _send(src, dst, send, recv, to):
    return pltpu.make_async_remote_copy(src_ref=src, dst_ref=dst, send_sem=send, recv_sem=recv, device_id={"tp": to},
                                        device_id_type=pl.DeviceIdType.MESH)


PIECE = 256
VMEM_LIMIT = 54 * 2**20
TILE = 256


def _kernel(x_ref, dy_ref, gain_ref, wq_ref, wk_ref, wv_ref, wo_ref, cl, sl, ch, sh,
            x_s, dgain_out, w_s, wo_s, a_out,
            a_s, dy_s, q_s, k_s, v_s, seent_s, do_s, top_s, mix_s, stat, dq_s, dk_s, dv_s, g_s, dg_s,
            send_sem, recv_sem, load_sem, a_sem, near_sem, over_send_sem, over_recv_sem, loc_sem, gain_send_sem, gain_recv_sem,
            at_sem, ready_sem):
    t, chip, core, over, beside = _ids()
    across = 2 * (1 - chip) + 1 - core
    peers = (over, beside, across)

    def state(way, n, block, to):
        at = a_s.at[_rows(block, n), :]
        return _send(at, at, send_sem.at[0, way, n], recv_sem.at[0, way, n], to)

    def dy_own(n, block):
        at = dy_s.at[_rows(block, n), :]
        return _send(at, at, send_sem.at[1, 1, n], recv_sem.at[1, 1, n], beside)

    def dy_piece(way, n, of_chip, half, to):
        block = 2 * of_chip + 1 - lax.div(n, 2)
        at = dy_s.at[pl.ds(pl.multiple_of(block * OWN + half * PIECE + lax.rem(n, 2) * CH, CH), CH), :]
        return _send(at, at, send_sem.at[1, way, n], recv_sem.at[1, way, n], to)

    loads = [pltpu.make_async_copy(src, dst, load_sem.at[i]) for i, (src, dst) in enumerate([
        (x_ref, x_s), (dy_ref, dy_s.at[_rows(t, 0, OWN), :]), (wq_ref, w_s.at[:, pl.ds(0, 512)]), (wk_ref, w_s.at[:, pl.ds(512, 256)]),
        (wv_ref, w_s.at[:, pl.ds(768, 256)]), (wo_ref, wo_s)])]
    for c in loads:
        c.start()
    _barrier(peers)
    loads[0].wait()

    gain = gain_ref[...].astype(F32).reshape(1, D)

    def norm(n, _):
        wide = x_s[pl.ds(pl.multiple_of(n * CH, CH), CH), :].astype(F32)
        scale = lax.rsqrt(jnp.mean(wide * wide, -1, keepdims=True) + 1e-6)
        a_s[_rows(t, n), :] = (wide * scale * gain).astype(BF)

        @pl.when(n >= 1)
        def _():
            state(0, n - 1, t, over).start()
            state(1, n - 1, t, beside).start()

    lax.fori_loop(0, NCH, norm, None)
    loads[1].wait()
    state(0, NCH - 1, t, over).start()
    state(1, NCH - 1, t, beside).start()
    for n in range(NCH):
        dy_own(n, t).start()
    for i in range(2, 6):
        loads[i].wait()

    def turn(u, cos, sin):
        a, b = u[:, :HALF].astype(BF).astype(F32), u[:, HALF:].astype(BF).astype(F32)
        return jnp.concatenate([a * cos - b * sin, b * cos + a * sin], -1).astype(BF)

    def unturn(g, cos, sin):
        g = g.astype(BF).astype(F32)
        a, b = g[:, :HALF], g[:, HALF:]
        return jnp.concatenate([a * cos + b * sin, b * cos - a * sin], -1).astype(BF)

    def project(block, n):
        rows = _rows(block, n)
        cos, sin = _angles(cl, sl, ch, sh, block * NCH + n)
        u = jnp.dot(a_s[rows, :], w_s[...], preferred_element_type=F32)
        q_s[0, rows, :] = turn(u[:, :256], cos, sin)
        q_s[1, rows, :] = turn(u[:, 256:512], cos, sin)
        k_s[rows, :] = turn(u[:, 512:768], cos, sin)
        v_s[rows, :] = u[:, 768:].astype(BF)

    def grad_seen(block):
        rows = _rows(block, 0, OWN)
        u = _dot(dy_s[rows, :], wo_s[...], 1, 1)
        do_s[0, rows, :] = u[:, :256].astype(BF)
        do_s[1, rows, :] = u[:, 256:].astype(BF)

    def deltas(block):
        def some(n, _):
            rows = _rows(block, n)
            for h in range(2):
                prod = do_s[h, rows, :].astype(F32) * g_s[rows, pl.ds(h * HEAD, HEAD)].astype(F32)
                stat[2 + h : 3 + h, rows] = prod.T.sum(axis=0, keepdims=True)

        lax.fori_loop(0, NCH, some, None)

    lax.fori_loop(0, NCH, lambda n, _: project(t, n), None)
    for n in range(NCH):
        dy_own(n, beside).wait_recv()
    for n in range(NCH):
        dy_piece(0, n, chip, core, over).start()

    def other(n, _):
        state(1, n, beside, beside).wait_recv()
        project(beside, n)

    lax.fori_loop(0, NCH, other, None)
    lax.fori_loop(0, 2, lambda m, _: grad_seen(2 * chip + m), None)
    dk_s[...] = jnp.zeros_like(dk_s)
    dv_s[...] = jnp.zeros_like(dv_s)

    def arrive(n, _):
        state(0, n, over, over).wait_recv()
        state(2, n, over, beside).start()
        project(over, n)
        state(2, n, across, beside).wait_recv()
        project(across, n)

    lax.fori_loop(0, NCH, arrive, None)
    a_store = pltpu.make_async_copy(a_s, a_out, a_sem)
    a_store.start()

    def hide(s, other):
        ok = lax.broadcasted_iota(jnp.int32, (OWN, OWN), 1) >= lax.broadcasted_iota(jnp.int32, (OWN, OWN), 0)
        return jnp.where(ok, s, other)

    def queries(i, _):
        rows = _rows(i, 0, OWN)
        top_s[...] = jnp.full((2, OWN), NEG, F32)
        mix_s[...] = jnp.zeros((2, HEAD + 8, OWN), F32)

        def block(j, masked):
            here = _rows(j, 0, OWN)
            keys = k_s[here, :]
            scores = [_dot(keys, q_s[h, rows, :], 1, 1) for h in range(2)]
            values = jnp.concatenate([v_s[here, :].T, jnp.ones((8, OWN), BF)], 0)
            weights, keeps = [], []
            for h in range(2):
                s = hide(scores[h], HIDDEN) if masked else scores[h]
                old = top_s[h : h + 1, :]
                top = jnp.maximum(old, s.max(axis=0, keepdims=True))
                top_s[h : h + 1, :] = top
                weights.append(jnp.exp2((s - top) * E2).astype(BF))
                keeps.append(jnp.exp2((old - top) * E2))
            for h in range(2):
                mix_s[h] = mix_s[h] * keeps[h] + _dot(values, weights[h], 1, 0)

        lax.fori_loop(0, i, lambda j, _: block(j, False), None)
        block(i, True)
        for h in range(2):
            total = mix_s[h, HEAD : HEAD + 1, :]
            out = mix_s[h, :HEAD, :] * (1 / total)
            seent_s[pl.ds(h * HEAD, HEAD), rows] = out.astype(BF)
            g_s[rows, pl.ds(h * HEAD, HEAD)] = out.T.astype(BF)
            stat[h : h + 1, rows] = top_s[h : h + 1, :] * E2 + jnp.log2(total)

    lax.fori_loop(0, ROWS // OWN, queries, None)

    def sent(n, _):
        state(0, n, t, over).wait_send()
        state(1, n, t, beside).wait_send()
        state(2, n, over, beside).wait_send()

    lax.fori_loop(0, NCH, sent, None)
    a_store.wait()
    for p in peers:
        pl.semaphore_signal(ready_sem, inc=1, device_id={"tp": p}, device_id_type=pl.DeviceIdType.MESH)
    near_at = lambda u: a_s.at[pl.ds(u * PIECE, PIECE), :]
    near_in = lambda u: a_s.at[pl.ds(OWN + u * PIECE, PIECE), :]
    over_at = 2 * OWN
    loc_in = a_s.at[pl.ds(3 * OWN, OWN), :]

    def pair(i, j, masked):
        cols, here = _rows(i, 0, OWN), _rows(j, 0, OWN)
        keys, values = k_s[here, :], v_s[here, :]
        qs = [q_s[h, cols, :] for h in range(2)]
        dos = [do_s[h, cols, :] for h in range(2)]
        scores = [_dot(keys, qs[h], 1, 1) for h in range(2)]
        dps = [_dot(values, dos[h], 1, 1) for h in range(2)]
        ps, dss = [], []
        for h in range(2):
            p = jnp.exp2(scores[h] * E2 - stat[h : h + 1, cols])
            p = hide(p, 0.0) if masked else p
            dss.append((p * (dps[h] - stat[2 + h : 3 + h, cols])).astype(BF))
            ps.append(p.astype(BF))
        dv_s[here, :] += _dot(jnp.concatenate(ps, 1), jnp.concatenate(dos, 0), 1, 0)
        dk_s[here, :] += _dot(jnp.concatenate(dss, 1), jnp.concatenate(qs, 0), 1, 0)
        turned_keys = keys.T
        for h in range(2):
            dq_s[h] += _dot(turned_keys, dss[h], 1, 0)

    def queries_back(i):
        deltas(i)
        dq_s[...] = jnp.zeros_like(dq_s)
        lax.fori_loop(0, i, lambda j, _: pair(i, j, False), None)
        pair(i, i, True)
        for n in range(NCH):
            rows = _rows(i, n)
            cos, sin = _angles(cl, sl, ch, sh, i * NCH + n)
            for h in range(2):
                g_s[rows, pl.ds(h * HEAD, HEAD)] = unturn((dq_s[h, :, n * CH : (n + 1) * CH] * SCALE).T, cos, sin)

    def keys_done(block):
        def some(n, _):
            rows = _rows(block, n)
            cos, sin = _angles(cl, sl, ch, sh, block * NCH + n)
            g_s[rows, pl.ds(512, HEAD)] = unturn(dk_s[rows, :] * SCALE, cos, sin)
            g_s[rows, pl.ds(768, HEAD)] = dv_s[rows, :].astype(BF)

        lax.fori_loop(0, NCH, some, None)

    def term(block, half):
        return _dot(g_s[_rows(block, half, PIECE), :], w_s[...], 1, 1)

    def near(u):
        return _send(near_at(u), near_in(u), near_sem.at[0, u], near_sem.at[1, u], beside)

    def to_owner(u, n):
        return _send(a_s.at[pl.ds(pl.multiple_of(u * PIECE + n * CH, CH), CH), :],
                     a_s.at[pl.ds(pl.multiple_of(over_at + core * PIECE + n * CH, CH), CH), :],
                     over_send_sem.at[u, n], over_recv_sem.at[core, n], 2 * (1 - chip) + 1 - u)

    def from_over(half, n):
        rows = a_s.at[pl.ds(over_at + half * PIECE + n * CH, CH), :]
        return _send(rows, rows, over_send_sem.at[0, n], over_recv_sem.at[half, n], over)

    def local():
        return _send(x_s, loc_in, loc_sem.at[0], loc_sem.at[1], beside)

    lax.fori_loop(0, 2, lambda m, _: queries_back(2 * chip + m), None)
    pl.semaphore_wait(ready_sem, 3)

    def far(u, _):
        block = 2 * (1 - chip) + 1 - u
        for m in range(2):
            dy_piece(0, 2 * u + m, 1 - chip, core, over).wait_recv()
            dy_piece(2, 2 * u + m, 1 - chip, core, beside).start()
        for m in range(2):
            dy_piece(2, 2 * u + m, 1 - chip, 1 - core, beside).wait_recv()
        grad_seen(block)
        queries_back(block)
        keys_done(block)
        near_at(u)[...] = term(block, 1 - core).astype(BF)
        near(u).start()
        mine = term(block, core)
        near(u).wait()
        near_at(u)[...] = (mine + near_in(u)[...].astype(F32)).astype(BF)
        for n in range(PIECE // CH):
            to_owner(u, n).start()

    lax.fori_loop(0, 2, far, None)

    def a_tile(i, slot):
        return pltpu.make_async_copy(a_out.at[:, pl.ds(pl.multiple_of(i * TILE, TILE), TILE)], do_s.at[slot], at_sem.at[slot])

    a_tile(0, 0).start()
    lax.fori_loop(0, 2, lambda m, _: keys_done(2 * chip + m), None)
    for half in range(2):
        x_s[pl.ds(half * PIECE, PIECE), :] = term(beside, half).astype(BF)
    local().start()
    own = lambda c, at, size: (dk_s.at[pl.ds(c * OWN + at, size), :] if c < 4 else dv_s.at[pl.ds((c - 4) * OWN + at, size), :] if c < 8
                               else dq_s.at[at // PIECE, pl.ds(at % PIECE, size), pl.ds(0, 256)])
    for half in range(2):
        mine = term(t, half)
        for c in range(D // 256):
            own(c, half * PIECE, PIECE)[...] = mine[:, c * 256 : (c + 1) * 256]

    def dw(i, _):
        slot = lax.rem(i, 2)

        @pl.when(i + 1 < D // TILE)
        def _():
            a_tile(i + 1, 1 - slot).start()

        a_tile(i, slot).wait()

        w_s[pl.ds(pl.multiple_of(i * TILE, TILE), TILE), :] = _dot(do_s[slot], g_s[...], 0, 0).astype(BF)

    lax.fori_loop(0, D // TILE, dw, None)
    local().wait()
    again = pltpu.make_async_copy(x_ref, x_s, load_sem.at[0])
    again.start()

    def dwo(i, _):
        columns = pl.ds(pl.multiple_of(i * TILE, TILE), TILE)
        wo_s[:, columns] = _dot(seent_s[...], dy_s[:, columns], 1, 0).astype(BF)

    lax.fori_loop(0, D // TILE, dwo, None)

    again.wait()
    dg_s[3] = jnp.zeros((1, D), F32)
    for n in range(PIECE // CH):
        for half in range(2):
            from_over(half, n).wait_recv()
            at = half * PIECE + n * CH
            rows = pl.ds(at, CH)
            mine = jnp.concatenate([own(c, at, CH)[...] for c in range(D // 256)], 1)
            da = mine + a_s[pl.ds(3 * OWN + at, CH), :].astype(F32) + a_s[pl.ds(over_at + at, CH), :].astype(F32)
            wide = x_s[rows, :].astype(F32)
            scale = lax.rsqrt(jnp.mean(wide * wide, -1, keepdims=True) + 1e-6)
            dg_s[3] += jnp.sum(da * wide * scale, 0, keepdims=True)
            da = da * gain
            pull = jnp.sum(da * wide, -1, keepdims=True) * scale * scale * scale * (-1 / D)
            x_s[rows, :] = (da * scale + pull * wide + dy_s[_rows(t, at // CH), :].astype(F32)).astype(BF)

    def gains(m):
        return _send(dg_s.at[3], dg_s.at[m], gain_send_sem.at[m], gain_recv_sem.at[m], peers[m])

    for m in range(3):
        gains(m).start()
    for m in range(3):
        gains(m).wait()
    dgain_out[...] = dg_s[3] + dg_s[0] + dg_s[1] + dg_s[2]
    for n in range(NCH):
        dy_own(n, t).wait_send()
        dy_piece(0, n, chip, core, over).wait_send()
        dy_piece(2, n, 1 - chip, core, beside).wait_send()
    for u in range(2):
        for n in range(PIECE // CH):
            to_owner(u, n).wait_send()


def _export(x_ref, gain_ref, w_ref, wo_ref, dx_out, dgain_out, dwq_out, dwk_out, dwv_out, dwo_out, sem):
    copies = [pltpu.make_async_copy(src, dst, sem.at[i]) for i, (src, dst) in enumerate([
        (w_ref.at[:, pl.ds(0, 512)], dwq_out), (w_ref.at[:, pl.ds(512, 256)], dwk_out), (w_ref.at[:, pl.ds(768, 256)], dwv_out),
        (wo_ref, dwo_out), (x_ref, dx_out), (gain_ref, dgain_out)])]
    for c in copies:
        c.start()
    for c in copies:
        c.wait()


def solution(mesh):
    vm = lambda s, d=BF: pltpu.VMEM(s, d)
    dma = lambda *s: pltpu.SemaphoreType.DMA(s)
    sds = jax.ShapeDtypeStruct

    def step(x, dy, gain, wq, wk, wv, wo):
        tables = [jnp.asarray(u) for u in _tables()]
        dx, dgain, dw, dwo, _ = pl.pallas_call(
            _kernel,
            out_shape=[vm((OWN, D)), vm((1, D), F32), vm((D, 1024)), vm((512, D)), sds((ROWS, D), BF)],
            in_specs=[ANY, ANY, VM, ANY, ANY, ANY, ANY, VM, VM, VM, VM],
            out_specs=[VM, VM, VM, VM, ANY],
            scratch_shapes=[
                vm((ROWS, D)), vm((ROWS, D)), vm((2, ROWS, HEAD)), vm((ROWS, HEAD)),
                vm((ROWS, HEAD)), vm((2 * HEAD, ROWS)), vm((2, ROWS, HEAD)), vm((2, OWN), F32), vm((2, HEAD + 8, OWN), F32),
                vm((8, ROWS), F32), vm((2, HEAD, OWN), F32), vm((ROWS, HEAD), F32), vm((ROWS, HEAD), F32), vm((ROWS, 1024)),
                vm((4, 1, D), F32),
                dma(2, 3, NCH), dma(2, 3, NCH), dma(6), pltpu.SemaphoreType.DMA, dma(2, 2), dma(2, 2), dma(2, 2), dma(2), dma(3), dma(3),
                dma(2), pltpu.SemaphoreType.REGULAR],
            compiler_params=pltpu.CompilerParams(collective_id=0, has_side_effects=True, vmem_limit_bytes=VMEM_LIMIT),
            name="half",
        )(x, dy, gain, wq, wk, wv, wo, *tables)
        held = [pltpu.with_memory_space_constraint(u, pltpu.VMEM) for u in (dx, dgain, dw, dwo)]
        return tuple(pl.pallas_call(
            _export,
            out_shape=[sds((OWN, D), BF), sds((1, D), F32), sds((D, 512), BF), sds((D, 256), BF), sds((D, 256), BF), sds((512, D), BF)],
            in_specs=[VM] * 4,
            out_specs=[ANY] * 6,
            scratch_shapes=[dma(6)],
            compiler_params=pltpu.CompilerParams(vmem_limit_bytes=2**20),
            name="export",
        )(*held))

    tokens, columns = P(("dp", "tp"), None), P(None, "tp")
    return jax.shard_map(
        step,
        mesh=mesh,
        in_specs=(tokens, tokens, P(None), columns, columns, columns, P("tp", None)),
        out_specs=(tokens, P("dp", None), P("dp", "tp"), P("dp", "tp"), P("dp", "tp"), P(("dp", "tp"), None)),
        check_vma=False,
    )
```

```python
import functools

import jax
import jax.numpy as jnp
import numpy as np
from jax import lax
from jax.experimental import pallas as pl
from jax.experimental.pallas import tpu as pltpu
from jax.sharding import PartitionSpec as P

HEAD = 256
HALF = HEAD // 2
THETA = 10000
LOG2E = 1.4426950408889634
NEG = -1e30
HIDDEN = 2 * NEG
ROWS = 2048
D = 2304
OWN = 512
CH = 128
NCH = OWN // CH
SCALE = HEAD**-0.5
E2 = SCALE * LOG2E
BF = jnp.bfloat16
F32 = jnp.float32
ANY = pl.BlockSpec(memory_space=pl.ANY)
VM = pl.BlockSpec(memory_space=pltpu.VMEM)


def _dot(a, b, ca, cb):
    return lax.dot_general(a, b, (((ca,), (cb,)), ((), ())), preferred_element_type=F32)


def _tables():
    freq = THETA ** (-np.arange(HALF) / HALF)
    low = np.arange(CH)[:, None] * freq
    high = (np.arange(ROWS // CH) * CH)[:, None] * freq
    return [np.asarray(f(t), np.float32) for t in (low, high) for f in (np.cos, np.sin)]


def _angles(cl, sl, ch, sh, block):
    c, s = ch[pl.ds(block, 1), :], sh[pl.ds(block, 1), :]
    return cl[...] * c - sl[...] * s, sl[...] * c + cl[...] * s


def _ids():
    t = lax.axis_index("tp")
    chip = lax.div(t, 2)
    core = t - 2 * chip
    return t, chip, core, 2 * (1 - chip) + core, 2 * chip + 1 - core


def _rows(block, n, size=CH):
    return pl.ds(pl.multiple_of(block * OWN + n * size, size), size)


def _send(src, dst, send, recv, to):
    return pltpu.make_async_remote_copy(src_ref=src, dst_ref=dst, send_sem=send, recv_sem=recv, device_id={"tp": to},
                                        device_id_type=pl.DeviceIdType.MESH)


PIECE = 256
VMEM_LIMIT = 54 * 2**20
LAST = 32
TILE = 256


def _kernel(x_ref, dy_ref, gain_ref, wq_ref, wk_ref, wv_ref, wo_ref, cl_ref, sl_ref, ch_ref, sh_ref,
            x_s, dgain_out, w_s, wo_s, a_out,
            gain_s, cl, sl, ch, sh, a_s, dy_s, q_s, k_s, v_s, seent_s, do_s, top_s, mix_s, stat, dq_s, dk_s, dv_s, g_s, dg_s,
            send_sem, recv_sem, x_sem, load_sem, a_sem, near_sem, over_send_sem, over_recv_sem, loc_sem, gain_send_sem, gain_recv_sem,
            at_sem, ready_sem):
    t, chip, core, over, beside = _ids()
    across = 2 * (1 - chip) + 1 - core
    peers = (over, beside, across)

    def state(way, n, block, to):
        at = a_s.at[_rows(block, n), :]
        return _send(at, at, send_sem.at[0, way, n], recv_sem.at[0, way, n], to)

    def dy_own(n, block):
        at = dy_s.at[_rows(block, n), :]
        return _send(at, at, send_sem.at[1, 1, n], recv_sem.at[1, 1, n], beside)

    def dy_piece(way, n, of_chip, half, to):
        block = 2 * of_chip + 1 - lax.div(n, 2)
        at = dy_s.at[pl.ds(pl.multiple_of(block * OWN + half * PIECE + lax.rem(n, 2) * CH, CH), CH), :]
        return _send(at, at, send_sem.at[1, way, n], recv_sem.at[1, way, n], to)

    x_loads = [pltpu.make_async_copy(x_ref.at[pl.ds(n * CH, CH), :], x_s.at[pl.ds(n * CH, CH), :], x_sem.at[n]) for n in range(NCH)]
    loads = [pltpu.make_async_copy(src, dst, load_sem.at[i]) for i, (src, dst) in enumerate([
        (dy_ref, dy_s.at[_rows(t, 0, OWN), :]), (wq_ref, w_s.at[:, pl.ds(0, 512)]), (wk_ref, w_s.at[:, pl.ds(512, 256)]),
        (wv_ref, w_s.at[:, pl.ds(768, 256)]), (wo_ref, wo_s), (cl_ref, cl), (sl_ref, sl), (ch_ref, ch), (sh_ref, sh)])]
    gain_load = pltpu.make_async_copy(gain_ref, gain_s, at_sem.at[0])
    gain_load.start()
    for c in x_loads:
        c.start()
    barrier = pltpu.get_barrier_semaphore()
    for p in peers:
        pl.semaphore_signal(barrier, inc=1, device_id={"tp": p}, device_id_type=pl.DeviceIdType.MESH)
    gain_load.wait()
    gain = gain_s[...].astype(F32).reshape(1, D)
    for n in range(NCH):
        x_loads[n].wait()
        wide = x_s[pl.ds(n * CH, CH), :].astype(F32)
        scale = lax.rsqrt(jnp.mean(wide * wide, -1, keepdims=True) + 1e-6)
        a_s[_rows(t, n), :] = (wide * scale * gain).astype(BF)
        if n == 1:
            pl.semaphore_wait(barrier, 3)
            for c in loads:
                c.start()
        if n >= 1:
            state(0, n - 1, t, over).start()
            state(1, n - 1, t, beside).start()
    loads[0].wait()
    state(0, NCH - 1, t, over).start()
    state(1, NCH - 1, t, beside).start()
    for n in range(NCH):
        dy_own(n, t).start()
    for c in loads[1:]:
        c.wait()

    def turn(u, cos, sin):
        a, b = u[:, :HALF].astype(BF).astype(F32), u[:, HALF:].astype(BF).astype(F32)
        return jnp.concatenate([a * cos - b * sin, b * cos + a * sin], -1).astype(BF)

    def unturn(g, cos, sin):
        g = g.astype(BF).astype(F32)
        a, b = g[:, :HALF], g[:, HALF:]
        return jnp.concatenate([a * cos + b * sin, b * cos - a * sin], -1).astype(BF)

    def project(block, n):
        rows = _rows(block, n)
        cos, sin = _angles(cl, sl, ch, sh, block * NCH + n)
        u = jnp.dot(a_s[rows, :], w_s[...], preferred_element_type=F32)
        q_s[0, rows, :] = turn(u[:, :256], cos, sin)
        q_s[1, rows, :] = turn(u[:, 256:512], cos, sin)
        k_s[rows, :] = turn(u[:, 512:768], cos, sin)
        v_s[rows, :] = u[:, 768:].astype(BF)

    def grad_seen(block):
        rows = _rows(block, 0, OWN)
        u = _dot(dy_s[rows, :], wo_s[...], 1, 1)
        do_s[0, rows, :] = u[:, :256].astype(BF)
        do_s[1, rows, :] = u[:, 256:].astype(BF)

    def deltas(block):
        def some(n, _):
            rows = _rows(block, n)
            for h in range(2):
                prod = do_s[h, rows, :].astype(F32) * g_s[rows, pl.ds(h * HEAD, HEAD)].astype(F32)
                stat[2 + h : 3 + h, rows] = prod.T.sum(axis=0, keepdims=True)

        lax.fori_loop(0, NCH, some, None)

    lax.fori_loop(0, NCH, lambda n, _: project(t, n), None)
    for n in range(NCH):
        dy_own(n, beside).wait_recv()
    for n in range(NCH):
        dy_piece(0, n, chip, core, over).start()

    def other(n, _):
        state(1, n, beside, beside).wait_recv()
        project(beside, n)

    lax.fori_loop(0, NCH, other, None)
    lax.fori_loop(0, 2, lambda m, _: grad_seen(2 * chip + m), None)
    dk_s[...] = jnp.zeros_like(dk_s)
    dv_s[...] = jnp.zeros_like(dv_s)

    def arrive(n, _):
        state(0, n, over, over).wait_recv()
        state(2, n, over, beside).start()
        project(over, n)
        state(2, n, across, beside).wait_recv()
        project(across, n)

    lax.fori_loop(0, NCH, arrive, None)
    a_store = pltpu.make_async_copy(a_s, a_out, a_sem)
    a_store.start()

    def hide(s, other):
        ok = lax.broadcasted_iota(jnp.int32, (OWN, OWN), 1) >= lax.broadcasted_iota(jnp.int32, (OWN, OWN), 0)
        return jnp.where(ok, s, other)

    def queries(i, _):
        rows = _rows(i, 0, OWN)
        top_s[...] = jnp.full((2, OWN), NEG, F32)
        mix_s[...] = jnp.zeros((2, HEAD + 8, OWN), F32)

        def block(j, masked):
            here = _rows(j, 0, OWN)
            keys = k_s[here, :]
            scores = [_dot(keys, q_s[h, rows, :], 1, 1) for h in range(2)]
            values = jnp.concatenate([v_s[here, :].T, jnp.ones((8, OWN), BF)], 0)
            weights, keeps = [], []
            for h in range(2):
                s = hide(scores[h], HIDDEN) if masked else scores[h]
                old = top_s[h : h + 1, :]
                top = jnp.maximum(old, s.max(axis=0, keepdims=True))
                top_s[h : h + 1, :] = top
                weights.append(jnp.exp2((s - top) * E2).astype(BF))
                keeps.append(jnp.exp2((old - top) * E2))
            for h in range(2):
                mix_s[h] = mix_s[h] * keeps[h] + _dot(values, weights[h], 1, 0)

        lax.fori_loop(0, i, lambda j, _: block(j, False), None)
        block(i, True)
        for h in range(2):
            total = mix_s[h, HEAD : HEAD + 1, :]
            out = mix_s[h, :HEAD, :] * (1 / total)
            seent_s[pl.ds(h * HEAD, HEAD), rows] = out.astype(BF)
            g_s[rows, pl.ds(h * HEAD, HEAD)] = out.T.astype(BF)
            stat[h : h + 1, rows] = top_s[h : h + 1, :] * E2 + jnp.log2(total)

    lax.fori_loop(0, ROWS // OWN, queries, None)

    def sent(n, _):
        state(0, n, t, over).wait_send()
        state(1, n, t, beside).wait_send()
        state(2, n, over, beside).wait_send()

    lax.fori_loop(0, NCH, sent, None)
    a_store.wait()
    for p in peers:
        pl.semaphore_signal(ready_sem, inc=1, device_id={"tp": p}, device_id_type=pl.DeviceIdType.MESH)
    near_at = lambda u: a_s.at[pl.ds(u * PIECE, PIECE), :]
    near_in = lambda u: a_s.at[pl.ds(OWN + u * PIECE, PIECE), :]
    over_at = 2 * OWN
    loc_in = a_s.at[pl.ds(3 * OWN, OWN), :]

    def pair(i, j, masked):
        cols, here = _rows(i, 0, OWN), _rows(j, 0, OWN)
        keys, values = k_s[here, :], v_s[here, :]
        qs = [q_s[h, cols, :] for h in range(2)]
        dos = [do_s[h, cols, :] for h in range(2)]
        scores = [_dot(keys, qs[h], 1, 1) for h in range(2)]
        dps = [_dot(values, dos[h], 1, 1) for h in range(2)]
        ps, dss = [], []
        for h in range(2):
            p = jnp.exp2(scores[h] * E2 - stat[h : h + 1, cols])
            p = hide(p, 0.0) if masked else p
            dss.append((p * (dps[h] - stat[2 + h : 3 + h, cols])).astype(BF))
            ps.append(p.astype(BF))
        dv_s[here, :] += _dot(jnp.concatenate(ps, 1), jnp.concatenate(dos, 0), 1, 0)
        dk_s[here, :] += _dot(jnp.concatenate(dss, 1), jnp.concatenate(qs, 0), 1, 0)
        turned_keys = keys.T
        for h in range(2):
            dq_s[h] += _dot(turned_keys, dss[h], 1, 0)

    def queries_back(i):
        deltas(i)
        dq_s[...] = jnp.zeros_like(dq_s)
        lax.fori_loop(0, i, lambda j, _: pair(i, j, False), None)
        pair(i, i, True)
        for n in range(NCH):
            rows = _rows(i, n)
            cos, sin = _angles(cl, sl, ch, sh, i * NCH + n)
            for h in range(2):
                g_s[rows, pl.ds(h * HEAD, HEAD)] = unturn((dq_s[h, :, n * CH : (n + 1) * CH] * SCALE).T, cos, sin)

    def keys_done(block):
        def some(n, _):
            rows = _rows(block, n)
            cos, sin = _angles(cl, sl, ch, sh, block * NCH + n)
            g_s[rows, pl.ds(512, HEAD)] = unturn(dk_s[rows, :] * SCALE, cos, sin)
            g_s[rows, pl.ds(768, HEAD)] = dv_s[rows, :].astype(BF)

        lax.fori_loop(0, NCH, some, None)

    def term(block, half):
        return _dot(g_s[_rows(block, half, PIECE), :], w_s[...], 1, 1)

    def near(u):
        return _send(near_at(u), near_in(u), near_sem.at[0, u], near_sem.at[1, u], beside)

    def to_owner(u, n):
        return _send(a_s.at[pl.ds(pl.multiple_of(u * PIECE + n * LAST, LAST), LAST), :],
                     a_s.at[pl.ds(pl.multiple_of(over_at + core * PIECE + n * LAST, LAST), LAST), :],
                     over_send_sem.at[u, n], over_recv_sem.at[core, n], 2 * (1 - chip) + 1 - u)

    def from_over(half, n):
        rows = a_s.at[pl.ds(pl.multiple_of(over_at + half * PIECE + n * LAST, LAST), LAST), :]
        return _send(rows, rows, over_send_sem.at[0, n], over_recv_sem.at[half, n], over)

    def local():
        return _send(x_s, loc_in, loc_sem.at[0], loc_sem.at[1], beside)

    lax.fori_loop(0, 2, lambda m, _: queries_back(2 * chip + m), None)
    pl.semaphore_wait(ready_sem, 3)

    def far(u, _):
        block = 2 * (1 - chip) + 1 - u
        for m in range(2):
            dy_piece(0, 2 * u + m, 1 - chip, core, over).wait_recv()
            dy_piece(2, 2 * u + m, 1 - chip, core, beside).start()
        for m in range(2):
            dy_piece(2, 2 * u + m, 1 - chip, 1 - core, beside).wait_recv()
        grad_seen(block)
        queries_back(block)
        keys_done(block)
        near_at(u)[...] = term(block, 1 - core).astype(BF)
        near(u).start()
        mine = term(block, core)
        near(u).wait()
        near_at(u)[...] = (mine + near_in(u)[...].astype(F32)).astype(BF)
        for n in range(PIECE // LAST):
            to_owner(u, n).start()

    lax.fori_loop(0, 2, far, None)

    def a_tile(i, slot):
        return pltpu.make_async_copy(a_out.at[:, pl.ds(pl.multiple_of(i * TILE, TILE), TILE)], do_s.at[slot], at_sem.at[slot])

    a_tile(0, 0).start()
    lax.fori_loop(0, 2, lambda m, _: keys_done(2 * chip + m), None)
    for half in range(2):
        x_s[pl.ds(half * PIECE, PIECE), :] = term(beside, half).astype(BF)
    local().start()
    def own(c, half, at, size):
        if c == 8:
            return dq_s.at[half, pl.ds(at, size), pl.ds(0, 256)]
        return (dk_s if c < 4 else dv_s).at[pl.ds(pl.multiple_of(c % 4 * OWN + half * PIECE + at, size), size), :]

    for half in range(2):
        mine = term(t, half)
        for c in range(D // 256):
            own(c, half, 0, PIECE)[...] = mine[:, c * 256 : (c + 1) * 256]

    def dw(i, _):
        slot = lax.rem(i, 2)

        @pl.when(i + 1 < D // TILE)
        def _():
            a_tile(i + 1, 1 - slot).start()

        a_tile(i, slot).wait()

        w_s[pl.ds(pl.multiple_of(i * TILE, TILE), TILE), :] = _dot(do_s[slot], g_s[...], 0, 0).astype(BF)

    lax.fori_loop(0, D // TILE, dw, None)
    local().wait()
    again = pltpu.make_async_copy(x_ref, x_s, x_sem.at[0])
    again.start()

    def dwo(i, _):
        columns = pl.ds(pl.multiple_of(i * TILE, TILE), TILE)
        wo_s[:, columns] = _dot(seent_s[...], dy_s[:, columns], 1, 0).astype(BF)

    lax.fori_loop(0, D // TILE, dwo, None)

    again.wait()
    dg_s[3] = jnp.zeros((1, D), F32)

    def whole(half, n):
        at = pl.multiple_of(n * LAST, LAST)
        rows = pl.ds(pl.multiple_of(half * PIECE + at, LAST), LAST)
        mine = jnp.concatenate([own(c, half, at, LAST)[...] for c in range(D // 256)], 1)
        for place in (3 * OWN, over_at):
            mine = mine + a_s[pl.ds(pl.multiple_of(place + half * PIECE + at, LAST), LAST), :].astype(F32)
        wide = x_s[rows, :].astype(F32)
        scale = lax.rsqrt(jnp.mean(wide * wide, -1, keepdims=True) + 1e-6)
        return rows, mine, wide, scale

    def by_gain(da, wide, scale):
        dg_s[3] += jnp.sum(da * wide * scale, 0, keepdims=True)

    def by_x(half, n, rows, da, wide, scale):
        da = da * gain
        pull = jnp.sum(da * wide, -1, keepdims=True) * scale * scale * scale * (-1 / D)
        dy = dy_s[pl.ds(pl.multiple_of(t * OWN + half * PIECE + n * LAST, LAST), LAST), :]
        x_s[rows, :] = (da * scale + pull * wide + dy.astype(F32)).astype(BF)

    def piece_in(n, _):
        for half in range(2):
            from_over(half, n).wait_recv()
            rows, *rest = whole(half, n)
            by_gain(*rest)
            by_x(half, n, rows, *rest)

    lax.fori_loop(0, PIECE // LAST - 1, piece_in, None)
    n = PIECE // LAST - 1
    for half in range(2):
        from_over(half, n).wait_recv()
        by_gain(*whole(half, n)[1:])

    def gains(m):
        return _send(dg_s.at[3], dg_s.at[m], gain_send_sem.at[m], gain_recv_sem.at[m], peers[m])

    for m in range(3):
        gains(m).start()
    for half in range(2):
        by_x(half, n, *whole(half, n))
    for m in range(3):
        gains(m).wait()
    dgain_out[...] = dg_s[3] + dg_s[0] + dg_s[1] + dg_s[2]
    for n in range(NCH):
        dy_own(n, t).wait_send()
        dy_piece(0, n, chip, core, over).wait_send()
        dy_piece(2, n, 1 - chip, core, beside).wait_send()
    for u in range(2):
        for n in range(PIECE // LAST):
            to_owner(u, n).wait_send()


def _export(x_ref, gain_ref, w_ref, wo_ref, dx_out, dgain_out, dwq_out, dwk_out, dwv_out, dwo_out, sem):
    copies = [pltpu.make_async_copy(src, dst, sem.at[i]) for i, (src, dst) in enumerate([
        (w_ref.at[:, pl.ds(0, 512)], dwq_out), (w_ref.at[:, pl.ds(512, 256)], dwk_out), (w_ref.at[:, pl.ds(768, 256)], dwv_out),
        (wo_ref, dwo_out), (x_ref, dx_out), (gain_ref, dgain_out)])]
    for c in copies:
        c.start()
    for c in copies:
        c.wait()


def solution(mesh):
    vm = lambda s, d=BF: pltpu.VMEM(s, d)
    dma = lambda *s: pltpu.SemaphoreType.DMA(s)
    sds = jax.ShapeDtypeStruct

    def step(x, dy, gain, wq, wk, wv, wo):
        tables = [jnp.asarray(u) for u in _tables()]
        dx, dgain, dw, dwo, _ = pl.pallas_call(
            _kernel,
            out_shape=[vm((OWN, D)), vm((1, D), F32), vm((D, 1024)), vm((512, D)), sds((ROWS, D), BF)],
            in_specs=[ANY] * 11,
            out_specs=[VM, VM, VM, VM, ANY],
            scratch_shapes=[
                vm((D,)), vm((CH, HALF), F32), vm((CH, HALF), F32), vm((ROWS // CH, HALF), F32), vm((ROWS // CH, HALF), F32), vm((ROWS, D)), vm((ROWS, D)), vm((2, ROWS, HEAD)), vm((ROWS, HEAD)),
                vm((ROWS, HEAD)), vm((2 * HEAD, ROWS)), vm((2, ROWS, HEAD)), vm((2, OWN), F32), vm((2, HEAD + 8, OWN), F32),
                vm((8, ROWS), F32), vm((2, HEAD, OWN), F32), vm((ROWS, HEAD), F32), vm((ROWS, HEAD), F32), vm((ROWS, 1024)),
                vm((4, 1, D), F32),
                dma(2, 3, NCH), dma(2, 3, NCH), dma(NCH), dma(9), pltpu.SemaphoreType.DMA, dma(2, 2), dma(2, PIECE // LAST), dma(2, PIECE // LAST), dma(2), dma(3), dma(3),
                dma(2), pltpu.SemaphoreType.REGULAR],
            compiler_params=pltpu.CompilerParams(collective_id=0, has_side_effects=True, vmem_limit_bytes=VMEM_LIMIT),
            name="half",
        )(x, dy, gain, wq, wk, wv, wo, *tables)
        held = [pltpu.with_memory_space_constraint(u, pltpu.VMEM) for u in (dx, dgain, dw, dwo)]
        return tuple(pl.pallas_call(
            _export,
            out_shape=[sds((OWN, D), BF), sds((1, D), F32), sds((D, 512), BF), sds((D, 256), BF), sds((D, 256), BF), sds((512, D), BF)],
            in_specs=[VM] * 4,
            out_specs=[ANY] * 6,
            scratch_shapes=[dma(6)],
            compiler_params=pltpu.CompilerParams(vmem_limit_bytes=2**20),
            name="export",
        )(*held))

    tokens, columns = P(("dp", "tp"), None), P(None, "tp")
    return jax.shard_map(
        step,
        mesh=mesh,
        in_specs=(tokens, tokens, P(None), columns, columns, columns, P("tp", None)),
        out_specs=(tokens, P("dp", None), P("dp", "tp"), P("dp", "tp"), P("dp", "tp"), P(("dp", "tp"), None)),
        check_vma=False,
    )
```

```python
import functools

import jax
import jax.numpy as jnp
import numpy as np
from jax import lax
from jax.experimental import pallas as pl
from jax.experimental.pallas import tpu as pltpu
from jax.sharding import PartitionSpec as P

HEAD = 256
HALF = HEAD // 2
THETA = 10000
LOG2E = 1.4426950408889634
NEG = -1e30
HIDDEN = 2 * NEG
ROWS = 2048
D = 2304
OWN = 512
CH = 128
NCH = OWN // CH
SCALE = HEAD**-0.5
E2 = SCALE * LOG2E
BF = jnp.bfloat16
F32 = jnp.float32
ANY = pl.BlockSpec(memory_space=pl.ANY)
VM = pl.BlockSpec(memory_space=pltpu.VMEM)


def _dot(a, b, ca, cb):
    return lax.dot_general(a, b, (((ca,), (cb,)), ((), ())), preferred_element_type=F32)


def _tables():
    freq = THETA ** (-np.arange(HALF) / HALF)
    low = np.arange(CH)[:, None] * freq
    high = (np.arange(ROWS // CH) * CH)[:, None] * freq
    return [np.asarray(f(t), np.float32) for t in (low, high) for f in (np.cos, np.sin)]


def _angles(cl, sl, ch, sh, block):
    c, s = ch[pl.ds(block, 1), :], sh[pl.ds(block, 1), :]
    return cl[...] * c - sl[...] * s, sl[...] * c + cl[...] * s


def _ids():
    t = lax.axis_index("tp")
    chip = lax.div(t, 2)
    core = t - 2 * chip
    return t, chip, core, 2 * (1 - chip) + core, 2 * chip + 1 - core


def _rows(block, n, size=CH):
    return pl.ds(pl.multiple_of(block * OWN + n * size, size), size)


def _send(src, dst, send, recv, to):
    return pltpu.make_async_remote_copy(src_ref=src, dst_ref=dst, send_sem=send, recv_sem=recv, device_id={"tp": to},
                                        device_id_type=pl.DeviceIdType.MESH)


PIECE = 256
VMEM_LIMIT = 54 * 2**20
EARLY = 32
LAST = 32
TILE = 256


def _kernel(x_ref, dy_ref, gain_ref, wq_ref, wk_ref, wv_ref, wo_ref, cl_ref, sl_ref, ch_ref, sh_ref,
            x_s, dgain_out, w_s, wo_s, a_out,
            gain_s, cl, sl, ch, sh, a_s, dy_s, q_s, k_s, v_s, seent_s, do_s, top_s, mix_s, stat, dq_s, dk_s, dv_s, g_s, dg_s,
            send_sem, recv_sem, x_sem, load_sem, a_sem, near_sem, over_send_sem, over_recv_sem, loc_sem,
            at_sem, early_sem, ready_sem):
    t, chip, core, over, beside = _ids()
    across = 2 * (1 - chip) + 1 - core
    peers = (over, beside, across)

    def state(way, n, block, to):
        at = a_s.at[_rows(block, n), :]
        return _send(at, at, send_sem.at[0, way], recv_sem.at[0, way, n], to)

    def dy_own(block):
        at = dy_s.at[_rows(block, 0, OWN), :]
        return _send(at, at, send_sem.at[1, 1], recv_sem.at[1, 1, 0], beside)

    def dy_rows(block, half, at, size):
        return pl.ds(pl.multiple_of(block * OWN + half * PIECE + at, EARLY), size)

    def dy_piece(way, pair, m, of_chip, half, to):
        skip = EARLY if way == 0 and m == 0 else 0
        at = dy_s.at[dy_rows(2 * of_chip + 1 - pair, half, m * CH + skip, CH - skip), :]
        n = 2 * pair + m
        return _send(at, at, send_sem.at[1, way], recv_sem.at[1, way, n], to)

    def dy_early(pair, of_chip, half, to, source=None):
        at = dy_s.at[dy_rows(2 * of_chip + 1 - pair, half, 0, EARLY), :]
        return _send(at if source is None else source, at, send_sem.at[1, 0], early_sem.at[pair], to)

    first = dy_early(1 - core, chip, core, over, dy_ref.at[pl.ds(pl.multiple_of(core * PIECE, EARLY), EARLY), :])
    second = dy_early(core, chip, core, over)

    x_loads = [pltpu.make_async_copy(x_ref.at[pl.ds(n * CH, CH), :], x_s.at[pl.ds(n * CH, CH), :], x_sem.at[n]) for n in range(NCH)]
    loads = [pltpu.make_async_copy(src, dst, load_sem.at[i]) for i, (src, dst) in enumerate([
        (dy_ref, dy_s.at[_rows(t, 0, OWN), :]), (wq_ref, w_s.at[:, pl.ds(0, 512)]), (wk_ref, w_s.at[:, pl.ds(512, 256)]),
        (wv_ref, w_s.at[:, pl.ds(768, 256)]), (wo_ref, wo_s), (cl_ref, cl), (sl_ref, sl), (ch_ref, ch), (sh_ref, sh)])]
    gain_load = pltpu.make_async_copy(gain_ref, gain_s, at_sem.at[0])
    gain_load.start()
    for c in x_loads:
        c.start()
    barrier = pltpu.get_barrier_semaphore()
    for p in peers:
        pl.semaphore_signal(barrier, inc=1, device_id={"tp": p}, device_id_type=pl.DeviceIdType.MESH)
    pl.semaphore_wait(barrier, 3)
    first.start()
    gain_load.wait()
    gain = gain_s[...].astype(F32).reshape(1, D)
    for n in range(NCH):
        x_loads[n].wait()
        wide = x_s[pl.ds(n * CH, CH), :].astype(F32)
        scale = lax.rsqrt(jnp.mean(wide * wide, -1, keepdims=True) + 1e-6)
        a_s[_rows(t, n), :] = (wide * scale * gain).astype(BF)
        if n == 1:
            for c in loads:
                c.start()
        if n >= 1:
            state(0, n - 1, t, over).start()
            state(1, n - 1, t, beside).start()
    loads[0].wait()
    state(0, NCH - 1, t, over).start()
    state(1, NCH - 1, t, beside).start()
    dy_own(t).start()
    for c in loads[1:]:
        c.wait()

    def turn(u, cos, sin):
        a, b = u[:, :HALF].astype(BF).astype(F32), u[:, HALF:].astype(BF).astype(F32)
        return jnp.concatenate([a * cos - b * sin, b * cos + a * sin], -1).astype(BF)

    def unturn(g, cos, sin):
        g = g.astype(BF).astype(F32)
        a, b = g[:, :HALF], g[:, HALF:]
        return jnp.concatenate([a * cos + b * sin, b * cos - a * sin], -1).astype(BF)

    def project(block, n):
        rows = _rows(block, n)
        cos, sin = _angles(cl, sl, ch, sh, block * NCH + n)
        u = jnp.dot(a_s[rows, :], w_s[...], preferred_element_type=F32)
        q_s[0, rows, :] = turn(u[:, :256], cos, sin)
        q_s[1, rows, :] = turn(u[:, 256:512], cos, sin)
        k_s[rows, :] = turn(u[:, 512:768], cos, sin)
        v_s[rows, :] = u[:, 768:].astype(BF)

    def grad_seen(block):
        rows = _rows(block, 0, OWN)
        u = _dot(dy_s[rows, :], wo_s[...], 1, 1)
        do_s[0, rows, :] = u[:, :256].astype(BF)
        do_s[1, rows, :] = u[:, 256:].astype(BF)

    def deltas(block):
        def some(n, _):
            rows = _rows(block, n)
            for h in range(2):
                prod = do_s[h, rows, :].astype(F32) * g_s[rows, pl.ds(h * HEAD, HEAD)].astype(F32)
                stat[2 + h : 3 + h, rows] = prod.T.sum(axis=0, keepdims=True)

        lax.fori_loop(0, NCH, some, None)

    lax.fori_loop(0, NCH, lambda n, _: project(t, n), None)
    dy_own(beside).wait_recv()
    second.start()
    for n in range(NCH):
        dy_piece(0, n // 2, n % 2, chip, core, over).start()

    def other(n, _):
        state(1, n, beside, beside).wait_recv()
        project(beside, n)

    lax.fori_loop(0, NCH, other, None)
    lax.fori_loop(0, 2, lambda m, _: grad_seen(2 * chip + m), None)
    dk_s[...] = jnp.zeros_like(dk_s)
    dv_s[...] = jnp.zeros_like(dv_s)

    def arrive(n, _):
        state(0, n, over, over).wait_recv()
        state(2, n, over, beside).start()
        project(over, n)
        state(2, n, across, beside).wait_recv()
        project(across, n)

    lax.fori_loop(0, NCH, arrive, None)
    a_store = pltpu.make_async_copy(a_s, a_out, a_sem)
    a_store.start()

    def hide(s, other):
        ok = lax.broadcasted_iota(jnp.int32, (OWN, OWN), 1) >= lax.broadcasted_iota(jnp.int32, (OWN, OWN), 0)
        return jnp.where(ok, s, other)

    def queries(i, _):
        rows = _rows(i, 0, OWN)
        top_s[...] = jnp.full((2, OWN), NEG, F32)
        mix_s[...] = jnp.zeros((2, HEAD + 8, OWN), F32)

        def block(j, masked):
            here = _rows(j, 0, OWN)
            keys = k_s[here, :]
            scores = [_dot(keys, q_s[h, rows, :], 1, 1) for h in range(2)]
            values = jnp.concatenate([v_s[here, :].T, jnp.ones((8, OWN), BF)], 0)
            weights, keeps = [], []
            for h in range(2):
                s = hide(scores[h], HIDDEN) if masked else scores[h]
                old = top_s[h : h + 1, :]
                top = jnp.maximum(old, s.max(axis=0, keepdims=True))
                top_s[h : h + 1, :] = top
                weights.append(jnp.exp2((s - top) * E2).astype(BF))
                keeps.append(jnp.exp2((old - top) * E2))
            for h in range(2):
                mix_s[h] = mix_s[h] * keeps[h] + _dot(values, weights[h], 1, 0)

        lax.fori_loop(0, i, lambda j, _: block(j, False), None)
        block(i, True)
        for h in range(2):
            total = mix_s[h, HEAD : HEAD + 1, :]
            out = mix_s[h, :HEAD, :] * (1 / total)
            seent_s[pl.ds(h * HEAD, HEAD), rows] = out.astype(BF)
            g_s[rows, pl.ds(h * HEAD, HEAD)] = out.T.astype(BF)
            stat[h : h + 1, rows] = top_s[h : h + 1, :] * E2 + jnp.log2(total)

    lax.fori_loop(0, ROWS // OWN, queries, None)

    def all_sent(kind, way):
        buf = (a_s, dy_s)[kind]
        at = buf.at[pl.ds(0, OWN), :]
        _send(at, at, send_sem.at[kind, way], recv_sem.at[kind, way, 0], over).wait_send()

    for way in range(3):
        all_sent(0, way)
    a_store.wait()
    for p in peers:
        pl.semaphore_signal(ready_sem, inc=1, device_id={"tp": p}, device_id_type=pl.DeviceIdType.MESH)
    near_at = lambda u: a_s.at[pl.ds(u * PIECE, PIECE), :]
    near_in = lambda u: a_s.at[pl.ds(OWN + u * PIECE, PIECE), :]
    over_at = 2 * OWN
    loc_in = a_s.at[pl.ds(3 * OWN, OWN), :]

    def pair(i, j, masked):
        cols, here = _rows(i, 0, OWN), _rows(j, 0, OWN)
        keys, values = k_s[here, :], v_s[here, :]
        qs = [q_s[h, cols, :] for h in range(2)]
        dos = [do_s[h, cols, :] for h in range(2)]
        scores = [_dot(keys, qs[h], 1, 1) for h in range(2)]
        dps = [_dot(values, dos[h], 1, 1) for h in range(2)]
        ps, dss = [], []
        for h in range(2):
            p = jnp.exp2(scores[h] * E2 - stat[h : h + 1, cols])
            p = hide(p, 0.0) if masked else p
            dss.append((p * (dps[h] - stat[2 + h : 3 + h, cols])).astype(BF))
            ps.append(p.astype(BF))
        dv_s[here, :] += _dot(jnp.concatenate(ps, 1), jnp.concatenate(dos, 0), 1, 0)
        dk_s[here, :] += _dot(jnp.concatenate(dss, 1), jnp.concatenate(qs, 0), 1, 0)
        turned_keys = keys.T
        for h in range(2):
            dq_s[h] += _dot(turned_keys, dss[h], 1, 0)

    def queries_back(i):
        deltas(i)
        dq_s[...] = jnp.zeros_like(dq_s)
        lax.fori_loop(0, i, lambda j, _: pair(i, j, False), None)
        pair(i, i, True)
        for n in range(NCH):
            rows = _rows(i, n)
            cos, sin = _angles(cl, sl, ch, sh, i * NCH + n)
            for h in range(2):
                g_s[rows, pl.ds(h * HEAD, HEAD)] = unturn((dq_s[h, :, n * CH : (n + 1) * CH] * SCALE).T, cos, sin)

    def keys_done(block):
        def some(n, _):
            rows = _rows(block, n)
            cos, sin = _angles(cl, sl, ch, sh, block * NCH + n)
            g_s[rows, pl.ds(512, HEAD)] = unturn(dk_s[rows, :] * SCALE, cos, sin)
            g_s[rows, pl.ds(768, HEAD)] = dv_s[rows, :].astype(BF)

        lax.fori_loop(0, NCH, some, None)

    def term(block, half):
        return _dot(g_s[_rows(block, half, PIECE), :], w_s[...], 1, 1)

    def near(u):
        return _send(near_at(u), near_in(u), near_sem.at[0, u], near_sem.at[1, u], beside)

    def to_owner(u, n):
        return _send(a_s.at[pl.ds(pl.multiple_of(u * PIECE + n * LAST, LAST), LAST), :],
                     a_s.at[pl.ds(pl.multiple_of(over_at + core * PIECE + n * LAST, LAST), LAST), :],
                     over_send_sem, over_recv_sem.at[core, n], 2 * (1 - chip) + 1 - u)

    def from_over(half, n):
        rows = a_s.at[pl.ds(pl.multiple_of(over_at + half * PIECE + n * LAST, LAST), LAST), :]
        return _send(rows, rows, over_send_sem, over_recv_sem.at[half, n], over)

    def local():
        return _send(x_s, loc_in, loc_sem.at[0], loc_sem.at[1], beside)

    lax.fori_loop(0, 2, lambda m, _: queries_back(2 * chip + m), None)
    pl.semaphore_wait(ready_sem, 3)

    def far(u, _):
        block = 2 * (1 - chip) + 1 - u
        for m in range(2):
            dy_piece(0, u, m, 1 - chip, core, over).wait_recv()
            if m == 0:
                dy_early(u, 1 - chip, core, over).wait_recv()
            dy_piece(2, u, m, 1 - chip, core, beside).start()
        for m in range(2):
            dy_piece(2, u, m, 1 - chip, 1 - core, beside).wait_recv()
        grad_seen(block)
        queries_back(block)
        keys_done(block)
        near_at(u)[...] = term(block, 1 - core).astype(BF)
        near(u).start()
        mine = term(block, core)
        near(u).wait()
        near_at(u)[...] = (mine + near_in(u)[...].astype(F32)).astype(BF)
        for n in range(PIECE // LAST):
            to_owner(u, n).start()

    lax.fori_loop(0, 2, far, None)

    def a_tile(i, slot):
        return pltpu.make_async_copy(a_out.at[:, pl.ds(pl.multiple_of(i * TILE, TILE), TILE)], do_s.at[slot], at_sem.at[slot])

    a_tile(0, 0).start()
    lax.fori_loop(0, 2, lambda m, _: keys_done(2 * chip + m), None)
    for half in range(2):
        x_s[pl.ds(half * PIECE, PIECE), :] = term(beside, half).astype(BF)
    local().start()
    def own(c, half, at, size):
        if c == 8:
            return dq_s.at[half, pl.ds(at, size), pl.ds(0, 256)]
        return (dk_s if c < 4 else dv_s).at[pl.ds(pl.multiple_of(c % 4 * OWN + half * PIECE + at, size), size), :]

    for half in range(2):
        mine = term(t, half)
        for c in range(D // 256):
            own(c, half, 0, PIECE)[...] = mine[:, c * 256 : (c + 1) * 256]

    def dw(i, _):
        slot = lax.rem(i, 2)

        @pl.when(i + 1 < D // TILE)
        def _():
            a_tile(i + 1, 1 - slot).start()

        a_tile(i, slot).wait()

        w_s[pl.ds(pl.multiple_of(i * TILE, TILE), TILE), :] = _dot(do_s[slot], g_s[...], 0, 0).astype(BF)

    lax.fori_loop(0, D // TILE, dw, None)
    local().wait()
    again = pltpu.make_async_copy(x_ref, x_s, x_sem.at[0])
    again.start()

    def dwo(i, _):
        columns = pl.ds(pl.multiple_of(i * TILE, TILE), TILE)
        wo_s[:, columns] = _dot(seent_s[...], dy_s[:, columns], 1, 0).astype(BF)

    lax.fori_loop(0, D // TILE, dwo, None)

    again.wait()
    dg_s[...] = jnp.zeros((1, D), F32)

    def whole(half, n):
        at = pl.multiple_of(n * LAST, LAST)
        rows = pl.ds(pl.multiple_of(half * PIECE + at, LAST), LAST)
        mine = jnp.concatenate([own(c, half, at, LAST)[...] for c in range(D // 256)], 1)
        for place in (3 * OWN, over_at):
            mine = mine + a_s[pl.ds(pl.multiple_of(place + half * PIECE + at, LAST), LAST), :].astype(F32)
        wide = x_s[rows, :].astype(F32)
        scale = lax.rsqrt(jnp.mean(wide * wide, -1, keepdims=True) + 1e-6)
        return rows, mine, wide, scale

    def by_gain(da, wide, scale):
        dg_s[...] += jnp.sum(da * wide * scale, 0, keepdims=True)

    def by_x(half, n, rows, da, wide, scale):
        da = da * gain
        pull = jnp.sum(da * wide, -1, keepdims=True) * scale * scale * scale * (-1 / D)
        dy = dy_s[pl.ds(pl.multiple_of(t * OWN + half * PIECE + n * LAST, LAST), LAST), :]
        x_s[rows, :] = (da * scale + pull * wide + dy.astype(F32)).astype(BF)

    def piece_in(n, _):
        for half in range(2):
            from_over(half, n).wait_recv()
            rows, *rest = whole(half, n)
            by_gain(*rest)
            by_x(half, n, rows, *rest)

    lax.fori_loop(0, PIECE // LAST - 1, piece_in, None)
    n = PIECE // LAST - 1
    for half in range(2):
        from_over(half, n).wait_recv()
        by_gain(*whole(half, n)[1:])

    for half in range(2):
        by_x(half, n, *whole(half, n))
    dgain_out[...] = dg_s[...]
    for way in range(3):
        all_sent(1, way)
    at = a_s.at[pl.ds(0, OWN), :]
    _send(at, at, over_send_sem, over_recv_sem.at[0, 0], over).wait_send()


def _export(x_ref, w_ref, wo_ref, dx_out, dwq_out, dwk_out, dwv_out, dwo_out, sem):
    copies = [pltpu.make_async_copy(src, dst, sem.at[i]) for i, (src, dst) in enumerate([
        (w_ref.at[:, pl.ds(0, 512)], dwq_out), (w_ref.at[:, pl.ds(512, 256)], dwk_out), (w_ref.at[:, pl.ds(768, 256)], dwv_out),
        (wo_ref, dwo_out), (x_ref, dx_out)])]
    for c in copies:
        c.start()
    for c in copies:
        c.wait()


def solution(mesh):
    vm = lambda s, d=BF: pltpu.VMEM(s, d)
    dma = lambda *s: pltpu.SemaphoreType.DMA(s)
    sds = jax.ShapeDtypeStruct

    def step(x, dy, gain, wq, wk, wv, wo):
        tables = [jnp.asarray(u) for u in _tables()]
        dx, dgain, dw, dwo, _ = pl.pallas_call(
            _kernel,
            out_shape=[vm((OWN, D)), sds((1, D), F32), vm((D, 1024)), vm((512, D)), sds((ROWS, D), BF)],
            in_specs=[ANY] * 11,
            out_specs=[VM, VM, VM, VM, ANY],
            scratch_shapes=[
                vm((D,)), vm((CH, HALF), F32), vm((CH, HALF), F32), vm((ROWS // CH, HALF), F32), vm((ROWS // CH, HALF), F32), vm((ROWS, D)), vm((ROWS, D)), vm((2, ROWS, HEAD)), vm((ROWS, HEAD)),
                vm((ROWS, HEAD)), vm((2 * HEAD, ROWS)), vm((2, ROWS, HEAD)), vm((2, OWN), F32), vm((2, HEAD + 8, OWN), F32),
                vm((8, ROWS), F32), vm((2, HEAD, OWN), F32), vm((ROWS, HEAD), F32), vm((ROWS, HEAD), F32), vm((ROWS, 1024)),
                vm((1, D), F32),
                dma(2, 3), dma(2, 3, NCH), dma(NCH), dma(9), pltpu.SemaphoreType.DMA, dma(2, 2), pltpu.SemaphoreType.DMA, dma(2, PIECE // LAST), dma(2),
                dma(2), dma(2), pltpu.SemaphoreType.REGULAR],
            compiler_params=pltpu.CompilerParams(collective_id=0, has_side_effects=True, vmem_limit_bytes=VMEM_LIMIT),
            name="half",
        )(x, dy, gain, wq, wk, wv, wo, *tables)
        others = [lax.ppermute(dgain, "tp", [(i, i ^ m) for i in range(4)]) for m in (1, 2, 3)]
        held = [pltpu.with_memory_space_constraint(u, pltpu.VMEM) for u in (dx, dw, dwo)]
        dx, *dws, dwo = pl.pallas_call(
            _export,
            out_shape=[sds((OWN, D), BF), sds((D, 512), BF), sds((D, 256), BF), sds((D, 256), BF), sds((512, D), BF)],
            in_specs=[VM] * 3,
            out_specs=[ANY] * 5,
            scratch_shapes=[dma(5)],
            compiler_params=pltpu.CompilerParams(vmem_limit_bytes=2**20),
            cost_estimate=pl.CostEstimate(flops=4 * 10**9, bytes_accessed=12 * 10**6, transcendentals=0),
            name="export",
        )(*held)
        return dx, (dgain + others[0]) + (others[1] + others[2]), *dws, dwo

    tokens, columns = P(("dp", "tp"), None), P(None, "tp")
    return jax.shard_map(
        step,
        mesh=mesh,
        in_specs=(tokens, tokens, P(None), columns, columns, columns, P("tp", None)),
        out_specs=(tokens, P("dp", None), P("dp", "tp"), P("dp", "tp"), P("dp", "tp"), P(("dp", "tp"), None)),
        check_vma=False,
    )
```

```python
import functools

import jax
import jax.numpy as jnp
import numpy as np
from jax import lax
from jax.experimental import pallas as pl
from jax.experimental.pallas import tpu as pltpu
from jax.sharding import PartitionSpec as P

HEAD = 256
HALF = HEAD // 2
THETA = 10000
LOG2E = 1.4426950408889634
NEG = -1e30
HIDDEN = 2 * NEG
ROWS = 2048
D = 2304
OWN = 512
CH = 128
NCH = OWN // CH
SCALE = HEAD**-0.5
E2 = SCALE * LOG2E
BF = jnp.bfloat16
F32 = jnp.float32
ANY = pl.BlockSpec(memory_space=pl.ANY)
VM = pl.BlockSpec(memory_space=pltpu.VMEM)


def _dot(a, b, ca, cb):
    return lax.dot_general(a, b, (((ca,), (cb,)), ((), ())), preferred_element_type=F32)


def _tables():
    freq = THETA ** (-np.arange(HALF) / HALF)
    low = np.arange(CH)[:, None] * freq
    high = (np.arange(ROWS // CH) * CH)[:, None] * freq
    return [np.asarray(f(t), np.float32) for t in (low, high) for f in (np.cos, np.sin)]


def _angles(cl, sl, ch, sh, block):
    c, s = ch[pl.ds(block, 1), :], sh[pl.ds(block, 1), :]
    return cl[...] * c - sl[...] * s, sl[...] * c + cl[...] * s


def _ids():
    t = lax.axis_index("tp")
    chip = lax.div(t, 2)
    core = t - 2 * chip
    return t, chip, core, 2 * (1 - chip) + core, 2 * chip + 1 - core


def _rows(block, n, size=CH):
    return pl.ds(pl.multiple_of(block * OWN + n * size, size), size)


def _send(src, dst, send, recv, to):
    return pltpu.make_async_remote_copy(src_ref=src, dst_ref=dst, send_sem=send, recv_sem=recv, device_id={"tp": to},
                                        device_id_type=pl.DeviceIdType.MESH)


PIECE = 256
VMEM_LIMIT = 54 * 2**20
EARLY = 32
LAST = 32
TILE = 256


def _kernel(x_ref, dy_ref, gain_ref, wq_ref, wk_ref, wv_ref, wo_ref, cl_ref, sl_ref, ch_ref, sh_ref,
            x_s, dgain_out, w_s, wo_s, a_out,
            gain_s, cl, sl, ch, sh, a_s, dy_s, q_s, k_s, v_s, seent_s, do_s, top_s, mix_s, stat, dq_s, dk_s, dv_s, g_s, dg_s,
            send_sem, recv_sem, x_sem, load_sem, a_sem, near_sem, over_send_sem, over_recv_sem, loc_sem,
            at_sem, early_sem, ready_sem):
    t, chip, core, over, beside = _ids()
    across = 2 * (1 - chip) + 1 - core
    peers = (over, beside, across)

    def state(way, n, block, to):
        at = a_s.at[_rows(block, n), :]
        return _send(at, at, send_sem.at[0, way], recv_sem.at[0, way, n], to)

    def dy_own(block):
        at = dy_s.at[_rows(block, 0, OWN), :]
        return _send(at, at, send_sem.at[1, 1], recv_sem.at[1, 1, 0], beside)

    def dy_rows(block, half, at, size):
        return pl.ds(pl.multiple_of(block * OWN + half * PIECE + at, EARLY), size)

    def dy_piece(way, pair, m, of_chip, half, to):
        skip = EARLY if way == 0 and m == 0 else 0
        at = dy_s.at[dy_rows(2 * of_chip + 1 - pair, half, m * CH + skip, CH - skip), :]
        n = 2 * pair + m
        return _send(at, at, send_sem.at[1, way], recv_sem.at[1, way, n], to)

    def dy_early(pair, of_chip, half, to, source=None):
        at = dy_s.at[dy_rows(2 * of_chip + 1 - pair, half, 0, EARLY), :]
        return _send(at if source is None else source, at, send_sem.at[1, 0], early_sem.at[pair], to)

    first = dy_early(1 - core, chip, core, over, dy_ref.at[pl.ds(pl.multiple_of(core * PIECE, EARLY), EARLY), :])
    second = dy_early(core, chip, core, over)

    x_loads = [pltpu.make_async_copy(x_ref.at[pl.ds(n * CH, CH), :], x_s.at[pl.ds(n * CH, CH), :], x_sem.at[n]) for n in range(NCH)]
    loads = [pltpu.make_async_copy(src, dst, load_sem.at[i]) for i, (src, dst) in enumerate([
        (dy_ref, dy_s.at[_rows(t, 0, OWN), :]), (wq_ref, w_s.at[:, pl.ds(0, 512)]), (wk_ref, w_s.at[:, pl.ds(512, 256)]),
        (wv_ref, w_s.at[:, pl.ds(768, 256)]), (wo_ref, wo_s), (cl_ref, cl), (sl_ref, sl), (ch_ref, ch), (sh_ref, sh)])]
    gain_load = pltpu.make_async_copy(gain_ref, gain_s, at_sem.at[0])
    gain_load.start()
    for c in x_loads:
        c.start()
    barrier = pltpu.get_barrier_semaphore()
    for p in peers:
        pl.semaphore_signal(barrier, inc=1, device_id={"tp": p}, device_id_type=pl.DeviceIdType.MESH)
    pl.semaphore_wait(barrier, 3)
    first.start()
    gain_load.wait()
    gain = gain_s[...].astype(F32).reshape(1, D)
    for n in range(NCH):
        x_loads[n].wait()
        wide = x_s[pl.ds(n * CH, CH), :].astype(F32)
        scale = lax.rsqrt(jnp.mean(wide * wide, -1, keepdims=True) + 1e-6)
        a_s[_rows(t, n), :] = (wide * scale * gain).astype(BF)
        if n == 1:
            for c in loads:
                c.start()
        if n >= 1:
            state(0, n - 1, t, over).start()
            state(1, n - 1, t, beside).start()
    loads[0].wait()
    state(0, NCH - 1, t, over).start()
    state(1, NCH - 1, t, beside).start()
    dy_own(t).start()
    for c in loads[1:]:
        c.wait()

    def turn(u, cos, sin):
        a, b = u[:, :HALF].astype(BF).astype(F32), u[:, HALF:].astype(BF).astype(F32)
        return jnp.concatenate([a * cos - b * sin, b * cos + a * sin], -1).astype(BF)

    def unturn(g, cos, sin):
        g = g.astype(BF).astype(F32)
        a, b = g[:, :HALF], g[:, HALF:]
        return jnp.concatenate([a * cos + b * sin, b * cos - a * sin], -1).astype(BF)

    def project(block, n):
        rows = _rows(block, n)
        cos, sin = _angles(cl, sl, ch, sh, block * NCH + n)
        u = jnp.dot(a_s[rows, :], w_s[...], preferred_element_type=F32)
        q_s[0, rows, :] = turn(u[:, :256], cos, sin)
        q_s[1, rows, :] = turn(u[:, 256:512], cos, sin)
        k_s[rows, :] = turn(u[:, 512:768], cos, sin)
        v_s[rows, :] = u[:, 768:].astype(BF)

    def grad_seen(block):
        rows = _rows(block, 0, OWN)
        u = _dot(dy_s[rows, :], wo_s[...], 1, 1)
        do_s[0, rows, :] = u[:, :256].astype(BF)
        do_s[1, rows, :] = u[:, 256:].astype(BF)

    def deltas(block):
        def some(n, _):
            rows = _rows(block, n)
            for h in range(2):
                prod = do_s[h, rows, :].astype(F32) * g_s[rows, pl.ds(h * HEAD, HEAD)].astype(F32)
                stat[2 + h : 3 + h, rows] = prod.T.sum(axis=0, keepdims=True)

        lax.fori_loop(0, NCH, some, None)

    lax.fori_loop(0, NCH, lambda n, _: project(t, n), None)
    dy_own(beside).wait_recv()
    second.start()
    for n in range(NCH):
        dy_piece(0, n // 2, n % 2, chip, core, over).start()

    def other(n, _):
        state(1, n, beside, beside).wait_recv()
        project(beside, n)

    lax.fori_loop(0, NCH, other, None)
    lax.fori_loop(0, 2, lambda m, _: grad_seen(2 * chip + m), None)
    dk_s[...] = jnp.zeros_like(dk_s)
    dv_s[...] = jnp.zeros_like(dv_s)

    def arrive(n, _):
        state(0, n, over, over).wait_recv()
        state(2, n, over, beside).start()
        project(over, n)
        state(2, n, across, beside).wait_recv()
        project(across, n)

    lax.fori_loop(0, NCH, arrive, None)
    a_store = pltpu.make_async_copy(a_s, a_out, a_sem)
    a_store.start()

    def hide(s, other):
        ok = lax.broadcasted_iota(jnp.int32, (OWN, OWN), 1) >= lax.broadcasted_iota(jnp.int32, (OWN, OWN), 0)
        return jnp.where(ok, s, other)

    def queries(i, _):
        rows = _rows(i, 0, OWN)
        top_s[...] = jnp.full((2, OWN), NEG, F32)
        mix_s[...] = jnp.zeros((2, HEAD + 8, OWN), F32)

        def block(j, masked):
            here = _rows(j, 0, OWN)
            keys = k_s[here, :]
            scores = [_dot(keys, q_s[h, rows, :], 1, 1) for h in range(2)]
            values = jnp.concatenate([v_s[here, :].T, jnp.ones((8, OWN), BF)], 0)
            weights, keeps = [], []
            for h in range(2):
                s = hide(scores[h], HIDDEN) if masked else scores[h]
                old = top_s[h : h + 1, :]
                top = jnp.maximum(old, s.max(axis=0, keepdims=True))
                top_s[h : h + 1, :] = top
                weights.append(jnp.exp2((s - top) * E2).astype(BF))
                keeps.append(jnp.exp2((old - top) * E2))
            for h in range(2):
                mix_s[h] = mix_s[h] * keeps[h] + _dot(values, weights[h], 1, 0)

        lax.fori_loop(0, i, lambda j, _: block(j, False), None)
        block(i, True)
        for h in range(2):
            total = mix_s[h, HEAD : HEAD + 1, :]
            out = mix_s[h, :HEAD, :] * (1 / total)
            seent_s[pl.ds(h * HEAD, HEAD), rows] = out.astype(BF)
            g_s[rows, pl.ds(h * HEAD, HEAD)] = out.T.astype(BF)
            stat[h : h + 1, rows] = top_s[h : h + 1, :] * E2 + jnp.log2(total)

    lax.fori_loop(0, ROWS // OWN, queries, None)

    def all_sent(kind, way):
        buf = (a_s, dy_s)[kind]
        at = buf.at[pl.ds(0, OWN), :]
        _send(at, at, send_sem.at[kind, way], recv_sem.at[kind, way, 0], over).wait_send()

    for way in range(3):
        all_sent(0, way)
    a_store.wait()
    for p in peers:
        pl.semaphore_signal(ready_sem, inc=1, device_id={"tp": p}, device_id_type=pl.DeviceIdType.MESH)
    near_at = lambda u: a_s.at[pl.ds(u * PIECE, PIECE), :]
    near_in = lambda u: a_s.at[pl.ds(OWN + u * PIECE, PIECE), :]
    over_at = 2 * OWN
    loc_in = a_s.at[pl.ds(3 * OWN, OWN), :]

    def pair(i, j, masked):
        cols, here = _rows(i, 0, OWN), _rows(j, 0, OWN)
        keys, values = k_s[here, :], v_s[here, :]
        qs = [q_s[h, cols, :] for h in range(2)]
        dos = [do_s[h, cols, :] for h in range(2)]
        scores = [_dot(keys, qs[h], 1, 1) for h in range(2)]
        dps = [_dot(values, dos[h], 1, 1) for h in range(2)]
        ps, dss = [], []
        for h in range(2):
            p = jnp.exp2(scores[h] * E2 - stat[h : h + 1, cols])
            p = hide(p, 0.0) if masked else p
            dss.append((p * (dps[h] - stat[2 + h : 3 + h, cols])).astype(BF))
            ps.append(p.astype(BF))
        dv_s[here, :] += _dot(jnp.concatenate(ps, 1), jnp.concatenate(dos, 0), 1, 0)
        dk_s[here, :] += _dot(jnp.concatenate(dss, 1), jnp.concatenate(qs, 0), 1, 0)
        turned_keys = keys.T
        for h in range(2):
            dq_s[h] += _dot(turned_keys, dss[h], 1, 0)

    def queries_back(i):
        deltas(i)
        dq_s[...] = jnp.zeros_like(dq_s)
        lax.fori_loop(0, i, lambda j, _: pair(i, j, False), None)
        pair(i, i, True)
        for n in range(NCH):
            rows = _rows(i, n)
            cos, sin = _angles(cl, sl, ch, sh, i * NCH + n)
            for h in range(2):
                g_s[rows, pl.ds(h * HEAD, HEAD)] = unturn((dq_s[h, :, n * CH : (n + 1) * CH] * SCALE).T, cos, sin)

    def keys_done(block):
        def some(n, _):
            rows = _rows(block, n)
            cos, sin = _angles(cl, sl, ch, sh, block * NCH + n)
            g_s[rows, pl.ds(512, HEAD)] = unturn(dk_s[rows, :] * SCALE, cos, sin)
            g_s[rows, pl.ds(768, HEAD)] = dv_s[rows, :].astype(BF)

        lax.fori_loop(0, NCH, some, None)

    def term(block, half):
        return _dot(g_s[_rows(block, half, PIECE), :], w_s[...], 1, 1)

    def near(u):
        return _send(near_at(u), near_in(u), near_sem.at[0, u], near_sem.at[1, u], beside)

    def to_owner(u, n):
        return _send(a_s.at[pl.ds(pl.multiple_of(u * PIECE + n * LAST, LAST), LAST), :],
                     a_s.at[pl.ds(pl.multiple_of(over_at + core * PIECE + n * LAST, LAST), LAST), :],
                     over_send_sem, over_recv_sem.at[core, n], 2 * (1 - chip) + 1 - u)

    def from_over(half, n):
        rows = a_s.at[pl.ds(pl.multiple_of(over_at + half * PIECE + n * LAST, LAST), LAST), :]
        return _send(rows, rows, over_send_sem, over_recv_sem.at[half, n], over)

    def local():
        return _send(x_s, loc_in, loc_sem.at[0], loc_sem.at[1], beside)

    lax.fori_loop(0, 2, lambda m, _: queries_back(2 * chip + m), None)
    pl.semaphore_wait(ready_sem, 3)

    def far(u, _):
        block = 2 * (1 - chip) + 1 - u
        for m in range(2):
            dy_piece(0, u, m, 1 - chip, core, over).wait_recv()
            if m == 0:
                dy_early(u, 1 - chip, core, over).wait_recv()
            dy_piece(2, u, m, 1 - chip, core, beside).start()
        for m in range(2):
            dy_piece(2, u, m, 1 - chip, 1 - core, beside).wait_recv()
        grad_seen(block)
        queries_back(block)
        keys_done(block)
        near_at(u)[...] = term(block, 1 - core).astype(BF)
        near(u).start()
        mine = term(block, core)
        near(u).wait()
        near_at(u)[...] = (mine + near_in(u)[...].astype(F32)).astype(BF)
        for n in range(PIECE // LAST):
            to_owner(u, n).start()

    lax.fori_loop(0, 2, far, None)

    def a_tile(i, slot):
        return pltpu.make_async_copy(a_out.at[:, pl.ds(pl.multiple_of(i * TILE, TILE), TILE)], do_s.at[slot], at_sem.at[slot])

    a_tile(0, 0).start()
    lax.fori_loop(0, 2, lambda m, _: keys_done(2 * chip + m), None)
    for half in range(2):
        x_s[pl.ds(half * PIECE, PIECE), :] = term(beside, half).astype(BF)
    local().start()
    def own(c, half, at, size):
        if c == 8:
            return dq_s.at[half, pl.ds(at, size), pl.ds(0, 256)]
        return (dk_s if c < 4 else dv_s).at[pl.ds(pl.multiple_of(c % 4 * OWN + half * PIECE + at, size), size), :]

    for half in range(2):
        mine = term(t, half)
        for c in range(D // 256):
            own(c, half, 0, PIECE)[...] = mine[:, c * 256 : (c + 1) * 256]

    def dw(i, _):
        slot = lax.rem(i, 2)

        @pl.when(i + 1 < D // TILE)
        def _():
            a_tile(i + 1, 1 - slot).start()

        a_tile(i, slot).wait()

        w_s[pl.ds(pl.multiple_of(i * TILE, TILE), TILE), :] = _dot(do_s[slot], g_s[...], 0, 0).astype(BF)

    lax.fori_loop(0, D // TILE, dw, None)
    local().wait()
    again = pltpu.make_async_copy(x_ref, x_s, x_sem.at[0])
    again.start()

    def dwo(i, _):
        columns = pl.ds(pl.multiple_of(i * TILE, TILE), TILE)
        wo_s[:, columns] = _dot(seent_s[...], dy_s[:, columns], 1, 0).astype(BF)

    lax.fori_loop(0, D // TILE, dwo, None)

    again.wait()
    dg_s[...] = jnp.zeros((1, D), F32)

    def whole(half, n):
        at = pl.multiple_of(n * LAST, LAST)
        rows = pl.ds(pl.multiple_of(half * PIECE + at, LAST), LAST)
        mine = jnp.concatenate([own(c, half, at, LAST)[...] for c in range(D // 256)], 1)
        for place in (3 * OWN, over_at):
            mine = mine + a_s[pl.ds(pl.multiple_of(place + half * PIECE + at, LAST), LAST), :].astype(F32)
        wide = x_s[rows, :].astype(F32)
        scale = lax.rsqrt(jnp.mean(wide * wide, -1, keepdims=True) + 1e-6)
        return rows, mine, wide, scale

    def by_gain(da, wide, scale):
        dg_s[...] += jnp.sum(da * wide * scale, 0, keepdims=True)

    def by_x(half, n, rows, da, wide, scale):
        da = da * gain
        pull = jnp.sum(da * wide, -1, keepdims=True) * scale * scale * scale * (-1 / D)
        dy = dy_s[pl.ds(pl.multiple_of(t * OWN + half * PIECE + n * LAST, LAST), LAST), :]
        x_s[rows, :] = (da * scale + pull * wide + dy.astype(F32)).astype(BF)

    def piece_in(n, _):
        for half in range(2):
            from_over(half, n).wait_recv()
            rows, *rest = whole(half, n)
            by_gain(*rest)
            by_x(half, n, rows, *rest)

    lax.fori_loop(0, PIECE // LAST, piece_in, None)
    dgain_out[...] = dg_s[...]
    for way in range(3):
        all_sent(1, way)
    at = a_s.at[pl.ds(0, OWN), :]
    _send(at, at, over_send_sem, over_recv_sem.at[0, 0], over).wait_send()


def _export(x_ref, w_ref, wo_ref, dx_out, dwq_out, dwk_out, dwv_out, dwo_out, sem):
    copies = [pltpu.make_async_copy(src, dst, sem.at[i]) for i, (src, dst) in enumerate([
        (w_ref.at[:, pl.ds(0, 512)], dwq_out), (w_ref.at[:, pl.ds(512, 256)], dwk_out), (w_ref.at[:, pl.ds(768, 256)], dwv_out),
        (wo_ref, dwo_out), (x_ref, dx_out)])]
    for c in copies:
        c.start()
    for c in copies:
        c.wait()


def solution(mesh):
    vm = lambda s, d=BF: pltpu.VMEM(s, d)
    dma = lambda *s: pltpu.SemaphoreType.DMA(s)
    sds = jax.ShapeDtypeStruct

    def step(x, dy, gain, wq, wk, wv, wo):
        tables = [jnp.asarray(u) for u in _tables()]
        dx, dgain, dw, dwo, _ = pl.pallas_call(
            _kernel,
            out_shape=[vm((OWN, D)), sds((1, D), F32), vm((D, 1024)), vm((512, D)), sds((ROWS, D), BF)],
            in_specs=[ANY] * 11,
            out_specs=[VM, VM, VM, VM, ANY],
            scratch_shapes=[
                vm((D,)), vm((CH, HALF), F32), vm((CH, HALF), F32), vm((ROWS // CH, HALF), F32), vm((ROWS // CH, HALF), F32), vm((ROWS, D)), vm((ROWS, D)), vm((2, ROWS, HEAD)), vm((ROWS, HEAD)),
                vm((ROWS, HEAD)), vm((2 * HEAD, ROWS)), vm((2, ROWS, HEAD)), vm((2, OWN), F32), vm((2, HEAD + 8, OWN), F32),
                vm((8, ROWS), F32), vm((2, HEAD, OWN), F32), vm((ROWS, HEAD), F32), vm((ROWS, HEAD), F32), vm((ROWS, 1024)),
                vm((1, D), F32),
                dma(2, 3), dma(2, 3, NCH), dma(NCH), dma(9), pltpu.SemaphoreType.DMA, dma(2, 2), pltpu.SemaphoreType.DMA, dma(2, PIECE // LAST), dma(2),
                dma(2), dma(2), pltpu.SemaphoreType.REGULAR],
            compiler_params=pltpu.CompilerParams(collective_id=0, has_side_effects=True, vmem_limit_bytes=VMEM_LIMIT),
            name="half",
        )(x, dy, gain, wq, wk, wv, wo, *tables)
        others = [lax.ppermute(dgain, "tp", [(i, i ^ m) for i in range(4)]) for m in (1, 2, 3)]
        held = [pltpu.with_memory_space_constraint(u, pltpu.VMEM) for u in (dx, dw, dwo)]
        dx, *dws, dwo = pl.pallas_call(
            _export,
            out_shape=[sds((OWN, D), BF), sds((D, 512), BF), sds((D, 256), BF), sds((D, 256), BF), sds((512, D), BF)],
            in_specs=[VM] * 3,
            out_specs=[ANY] * 5,
            scratch_shapes=[dma(5)],
            compiler_params=pltpu.CompilerParams(vmem_limit_bytes=2**20),
            cost_estimate=pl.CostEstimate(flops=4 * 10**9, bytes_accessed=12 * 10**6, transcendentals=0),
            name="export",
        )(*held)
        return dx, (dgain + others[0]) + (others[1] + others[2]), *dws, dwo

    tokens, columns = P(("dp", "tp"), None), P(None, "tp")
    return jax.shard_map(
        step,
        mesh=mesh,
        in_specs=(tokens, tokens, P(None), columns, columns, columns, P("tp", None)),
        out_specs=(tokens, P("dp", None), P("dp", "tp"), P("dp", "tp"), P("dp", "tp"), P(("dp", "tp"), None)),
        check_vma=False,
    )
```
